32 devices in a mesh: groups: 2 (over x), wide: 16 (over z, y, core).
Axes of the slice: x: 2, y: 2, z: 4, core: 2. Of those that a mesh axis runs over, the one named last changes fastest.
Arguments:
- queries: bfloat16 [256, 3072], P(('groups', 'wide')), parts along dimension 0, may hold values from -15 to 15
- hidden_in: bfloat16 [256, 3072], P(('groups', 'wide')), parts along dimension 0, may hold values from -170 to 170
- prefix_keys: bfloat16 [16384, 512], P(('groups', 'wide')), parts along dimension 0, may hold values from -12 to 12
- prefix_values: bfloat16 [16384, 512], P(('groups', 'wide')), parts along dimension 0, may hold values from -24 to 24
- suffix_keys: bfloat16 [256, 64, 512], P(('groups', 'wide')), parts along dimension 0, may hold values from -21 to 21
- suffix_values: bfloat16 [256, 64, 512], P(('groups', 'wide')), parts along dimension 0, may hold values from -24 to 24
- suffix_length: int32 [256], P(('groups', 'wide')), parts along dimension 0, may hold values from 2 to 64, as said below
- prefix_of: int32 [256, 1], P('groups'), parts along dimension 0, may hold values from 0 to 7; in each aligned block of 8 rows (0 to 7, 8 to 15, ...) at most 2 rows name the same one
- expert_index: int32 [256, 2], P('groups'), parts along dimension 0, may hold values from 0 to 3, all different within a row; in each aligned block of 8 rows (0 to 7, 8 to 15, ...) at most 6 rows name the same one
- gate_logits: float32 [256, 2], P('groups'), parts along dimension 0, may hold values from -6 to 6
- norm_gain: float32 [3072], replicated, may hold values from 0.1 to 1.9
- gate_weight: bfloat16 [3072, 32768], P(None, 'wide'), may hold values from -0.109375 to 0.109375
- up_weight: bfloat16 [3072, 32768], P(None, 'wide'), may hold values from -0.109375 to 0.109375
- down_weight: bfloat16 [32768, 3072], P('wide'), may hold values from -0.125 to 0.125
Outputs:
- attended: bfloat16 [256, 3072], P(('groups', 'wide')), parts along dimension 0
- expert_mix: bfloat16 [256, 3072], P(('groups', 'wide')), parts along dimension 0
The draws below stay inside these ranges and needn't reach their ends.
There are 2 independent parts, one for each index of `groups`. The reference program is written for one: setup_inputs(seed, part) draws one part's arguments, and reference() takes and returns one part's arrays. A program takes and returns all parts, laid end to end along the dimension named above; an argument that names none is the same for every part. Nothing has to cross between parts.
Inputs may be any that keep to these rules, and one draw needn't show every extreme that they name: `prefix_of`: among the requests of one device at most 2 share a prefix; in some of the aligned blocks exactly 2 do. `expert_index`: each request names 2 different experts; among the requests of one device at most 6 name the same expert, and in some aligned blocks exactly 6 do. `suffix_length`: every device holds a request with 64 live suffix tokens.
All inputs are finite; a program needn't handle non-finite values.
Results may differ from the reference program's by a relative error of at most 0.0095.
Values may be sent and summed in bfloat16 or wider, within the bound.
No kernel may reach another device: no remote copies, remote signals or barrier semaphores. Data moves between devices by JAX's collectives and lax.ppermute only.
A program may use at most 128 MiB of HBM per device.

```python
import math
import jax
import jax.numpy as jnp
import numpy as np
from jax import lax

D = 3072
HQ = 24
HK = 4
DH = 128
FF = 8192
EXPERTS = 4
TOP = 2
PREFIXES = 8
PTOK_DEV = 512
REQ_DEV = 8
SMAX = 64
CAPP = 2
CAPE = 6
R = 128
PLEN = 1024


def draw_queries(key, part):
    values_out = jnp.clip(jax.random.normal(jax.random.fold_in(key, 11), (R, D), jnp.float32), -4.0, 4.0)
    return values_out.astype(jnp.bfloat16)


def draw_suffix_keys(key, part):
    values_out = jnp.clip(2.0 * jax.random.normal(jax.random.fold_in(key, 21), (R, SMAX, HK * DH), jnp.float32), -12.0, 12.0)
    return values_out.astype(jnp.bfloat16)


def draw_suffix_length(key, part):
    lengths = jax.random.randint(jax.random.fold_in(key, 31), (R,), 2, SMAX + 1)
    picked = jax.random.randint(jax.random.fold_in(key, 32), (R // REQ_DEV,), 0, REQ_DEV)
    position = jnp.arange(R)
    longest = position % REQ_DEV == picked[position // REQ_DEV]
    return jnp.where(longest, SMAX, lengths).astype(jnp.int32)


def draw_hidden_in(key, part):
    values_out = jnp.clip(jax.random.normal(jax.random.fold_in(key, 41), (R, D), jnp.float32), -5.0, 5.0)
    return values_out.astype(jnp.bfloat16)


def levels(own_key, shape, pieces, least, top_value):
    level = 1.0
    for dim, shards_of in pieces:
        draws = jax.random.uniform(jax.random.fold_in(jax.random.fold_in(own_key, 6), dim), (shards_of,), jnp.float32, least / len(pieces), top_value / len(pieces))
        level = level * jnp.repeat(jnp.exp(draws), shape[dim] // shards_of).reshape((-1,) + (1,) * (len(shape) - 1 - dim))
    return level


def deal_out(rng, own, number, rows, number_of, top, bound, skew):
    order = jax.random.permutation(rng, number_of)
    crowded, common = load_shares(number_of, rows * top, bound, skew, True), load_shares(number_of, rows * top, bound, skew, False)
    places = jnp.arange(number_of)

    def named(sizes, rotation):
        used = int((sizes > 0).sum())
        fixed = max(1, used // 4)
        shifted = fixed + (places - fixed + rotation * (used - fixed)) % max(1, number_of - fixed)
        return jnp.zeros((number_of,), jnp.int32).at[order[jnp.where(places < fixed, places, shifted)]].set(jnp.asarray(sizes, jnp.int32))

    sizes = jnp.where(number % 4 == 0, named(crowded, number // 4), named(common, number - number // 4 - 1))
    mixed = jax.random.permutation(jax.random.fold_in(own, 3), number_of)
    source_of, sink = mixed[0:number_of // 2 * 2:2], mixed[1:number_of // 2 * 2:2]
    slack = jnp.minimum(sizes[source_of] - 1, bound - sizes[sink]) // 2
    slack = jnp.where((source_of == order[0]) | (sink == order[0]) | (sizes[sink] == 0), 0, jnp.maximum(slack, 0))
    shifted = jax.random.randint(jax.random.fold_in(own, 4), (number_of // 2,), 0, 1 << 20) % (slack + 1)
    sizes = sizes.at[source_of].add(-shifted).at[sink].add(shifted)
    labels = jnp.searchsorted(jnp.cumsum(sizes), jnp.arange(rows * top), side="right").astype(jnp.int32)
    grid = labels.reshape(top, rows).T
    grid = grid[jax.random.permutation(jax.random.fold_in(own, 1), rows)]
    rotation = jax.random.randint(jax.random.fold_in(own, 2), (rows, 1), 0, top)
    return jnp.take_along_axis(grid, (jnp.arange(top)[None, :] + rotation) % top, axis=1)


def load_shares(count, total, most, slope, full):
    loads = [(1 << 20) // math.isqrt(grade ** slope) + 1 for grade in range(1, count + 1)]
    largest = most if full else min(most, max(-(-total // count), total * loads[0] // sum(loads)))
    least = 1 if total - largest >= count - 1 else 0
    counts, spare = [largest] + [least] * (count - 1), total - largest - least * (count - 1)
    while spare > 0:
        movable = [i for i in range(1, count) if counts[i] < largest] or [i for i in range(1, count) if counts[i] < most]
        pool, left = sum([loads[i] for i in movable]), spare
        for i in movable:
            more = min(most - counts[i], max(1, left * loads[i] // pool), spare)
            counts[i] = counts[i] + more
            spare = spare - more
    return np.array(counts)


def bell_draw(rng, shape, deviation, most, pieces=(), held_as=jnp.bfloat16):
    result = deviation * jax.random.normal(rng, shape, jnp.float32)
    if pieces:
        result = result * levels(rng, shape, pieces, -0.22, 0.18)
    return jnp.clip(result, -most, most).astype(held_as)


def setup_inputs(seed: int = 0, part: int = 0) -> dict:
    key_list = jax.random.split(jax.random.key(seed), 15)
    part_splits = jax.random.split(jax.random.fold_in(key_list[14], part), 15)
    queries = draw_queries(jax.random.fold_in(jax.random.fold_in(key_list[14], part), 71), part)
    hidden_in = draw_hidden_in(jax.random.fold_in(jax.random.fold_in(key_list[14], part), 71), part)
    prefix_keys = bell_draw(part_splits[2], (PREFIXES * PLEN, HK * DH), 2.0, 12.0, ((0, 16),))
    prefix_values = bell_draw(part_splits[3], (PREFIXES * PLEN, HK * DH), 4.0, 24.0, ((0, 16),))
    suffix_keys = draw_suffix_keys(jax.random.fold_in(jax.random.fold_in(key_list[14], part), 71), part)
    suffix_values = bell_draw(part_splits[5], (R, SMAX, HK * DH), 4.0, 24.0, ((0, 16),))
    suffix_length = draw_suffix_length(jax.random.fold_in(jax.random.fold_in(key_list[14], part), 71), part)
    prefix_of_keys = jax.random.split(jax.random.fold_in(part_splits[7], 1), R // REQ_DEV)
    prefix_of_turns = jax.random.permutation(jax.random.fold_in(part_splits[7], 3), R // REQ_DEV)
    prefix_of = jax.vmap(lambda own, number: deal_out(jax.random.fold_in(part_splits[7], 2), own, number, REQ_DEV, PREFIXES, 1, CAPP, 2))(prefix_of_keys, prefix_of_turns).reshape((R, 1))
    expert_index_keys = jax.random.split(jax.random.fold_in(part_splits[8], 1), R // REQ_DEV)
    expert_index_turns = jax.random.permutation(jax.random.fold_in(part_splits[8], 3), R // REQ_DEV)
    expert_index = jax.vmap(lambda own, number: deal_out(jax.random.fold_in(part_splits[8], 2), own, number, REQ_DEV, EXPERTS, TOP, CAPE, 2))(expert_index_keys, expert_index_turns).reshape((R, TOP))
    gate_logits = bell_draw(part_splits[9], (R, TOP), 1.0, 6.0, (), jnp.float32)
    norm_gain = jnp.clip(1.0 + 0.18 * jax.random.normal(key_list[10], (D,), jnp.float32), 0.1, 1.9)
    gate_weight = bell_draw(key_list[11], (D, EXPERTS * FF), D ** -0.5, 0.109375, ((1, 16),))
    up_weight = bell_draw(key_list[12], (D, EXPERTS * FF), D ** -0.5, 0.109375, ((1, 16),))
    down_weight = bell_draw(key_list[13], (EXPERTS * FF, D), (FF // 4) ** -0.5, 0.125, ((0, 16),))
    return dict(queries=queries, hidden_in=hidden_in, prefix_keys=prefix_keys, prefix_values=prefix_values, suffix_keys=suffix_keys, suffix_values=suffix_values, suffix_length=suffix_length, prefix_of=prefix_of, expert_index=expert_index, gate_logits=gate_logits, norm_gain=norm_gain, gate_weight=gate_weight, up_weight=up_weight, down_weight=down_weight)


masked_score = -1e+30

def reference(queries, hidden_in, prefix_keys, prefix_values, suffix_keys, suffix_values, suffix_length, prefix_of, expert_index, gate_logits, norm_gain, gate_weight, up_weight, down_weight):
    group_size = HQ // HK
    blocks = PLEN // PTOK_DEV
    score_scale = 1.0 / math.sqrt(DH)

    def one_request(packed):
        query_row, prefix_row, own_keys, own_values, length = packed
        query_heads = query_row.astype(jnp.float32).reshape(HK, group_size, DH)
        first_row = (prefix_row * PLEN).astype(jnp.int32)
        prefix_k = lax.dynamic_slice_in_dim(prefix_keys, first_row, PLEN, 0).astype(jnp.float32).reshape(blocks, PTOK_DEV, HK, DH)
        prefix_v = lax.dynamic_slice_in_dim(prefix_values, first_row, PLEN, 0).astype(jnp.float32).reshape(blocks, PTOK_DEV, HK, DH)
        scores = jnp.einsum('kgd,btkd->kgbt', query_heads, prefix_k) * score_scale
        block_max = lax.optimization_barrier(jnp.max(scores, axis=-1))
        weights = lax.optimization_barrier(jnp.exp(scores - block_max[..., None]).astype(jnp.bfloat16)).astype(jnp.float32)
        block_sum = lax.optimization_barrier(jnp.sum(weights, axis=-1))
        block_out = jnp.einsum('kgbt,btkd->kgbd', weights, prefix_v)
        suffix_k = own_keys.astype(jnp.float32).reshape(SMAX, HK, DH)
        suffix_v = own_values.astype(jnp.float32).reshape(SMAX, HK, DH)
        suffix_scores = jnp.einsum('kgd,skd->kgs', query_heads, suffix_k) * score_scale
        usable = jnp.arange(SMAX, dtype=jnp.int32) < length
        suffix_scores = jnp.where(usable, suffix_scores, masked_score)
        suffix_max = lax.optimization_barrier(jnp.max(suffix_scores, axis=-1))
        suffix_weights = lax.optimization_barrier(jnp.exp(suffix_scores - suffix_max[..., None]).astype(jnp.bfloat16)).astype(jnp.float32)
        suffix_sum = lax.optimization_barrier(jnp.sum(suffix_weights, axis=-1))
        suffix_out = jnp.einsum('kgs,skd->kgd', suffix_weights, suffix_v)
        overall = jnp.maximum(lax.optimization_barrier(jnp.max(block_max, axis=-1)), suffix_max)
        factors = jnp.exp(block_max - overall[..., None])
        suffix_factor = jnp.exp(suffix_max - overall)
        numerator = lax.optimization_barrier(jnp.sum(factors[..., None] * block_out, axis=2)) + suffix_factor[..., None] * suffix_out
        denominator = lax.optimization_barrier(jnp.sum(factors * block_sum, axis=-1)) + suffix_factor * suffix_sum
        return (numerator / denominator[..., None]).reshape(D).astype(jnp.bfloat16)
    attended = lax.map(one_request, (queries, prefix_of[:, 0], suffix_keys, suffix_values, suffix_length))
    stream = hidden_in.astype(jnp.float32) + attended.astype(jnp.float32)
    normed = (stream * lax.rsqrt(lax.optimization_barrier(jnp.mean(stream * stream, axis=-1, keepdims=True)) + 1e-05) * norm_gain).astype(jnp.bfloat16)
    gates = jax.nn.softmax(gate_logits, axis=-1)
    mixture = jnp.zeros((R, D), jnp.float32)
    for expert in range(EXPERTS):
        gate_part = jnp.dot(normed, gate_weight[:, expert * FF:(expert + 1) * FF], preferred_element_type=jnp.float32)
        up_part = jnp.dot(normed, up_weight[:, expert * FF:(expert + 1) * FF], preferred_element_type=jnp.float32)
        hidden = (jax.nn.silu(gate_part) * up_part).astype(jnp.bfloat16)
        expert_out = jnp.dot(hidden, down_weight[expert * FF:(expert + 1) * FF, :], preferred_element_type=jnp.float32)
        share = lax.optimization_barrier(jnp.sum(gates * (expert_index == expert).astype(jnp.float32), axis=1))
        mixture = mixture + share[:, None] * expert_out
    return (attended, mixture.astype(jnp.bfloat16))
```

```python
import math

import jax
import jax.numpy as jnp
from jax import lax
from jax.sharding import PartitionSpec as P

HQ = 24
HK = 4
DH = 128
EXPERTS = 4
PREFIXES = 8
CAPP = 2
STAT = 128

masked_score = -1e30


def split_parts(x, parts):
    pieces = []
    for _ in range(parts):
        piece = lax.reduce_precision(x, 8, 7)
        pieces.append(piece.astype(jnp.bfloat16))
        x = x - piece
    return pieces


def attend(query_rows, key_rows, value_rows):
    rows, width = query_rows.shape
    query_heads = query_rows.reshape(rows, HK, HQ // HK, DH)
    key_heads = key_rows.reshape(key_rows.shape[0], HK, DH)
    value_heads = value_rows.reshape(value_rows.shape[0], HK, DH)
    scores = jnp.einsum(
        "nkgd,pkd->nkgp", query_heads, key_heads, preferred_element_type=jnp.float32
    ) * (1.0 / math.sqrt(DH))
    block_max = jnp.max(scores, axis=-1)
    weights = jnp.exp(scores - block_max[..., None]).astype(jnp.bfloat16)
    block_sum = jnp.sum(weights.astype(jnp.float32), axis=-1)
    block_out = jnp.einsum(
        "nkgp,pkd->nkgd", weights, value_heads, preferred_element_type=jnp.float32
    )
    return block_out.reshape(rows, width), block_max.reshape(rows, HQ), block_sum.reshape(rows, HQ)


def attend_suffix(query_rows, key_rows, value_rows, lengths):
    rows = query_rows.shape[0]
    slots_max = key_rows.shape[1]
    query_heads = query_rows.reshape(rows, HK, HQ // HK, DH)
    key_heads = key_rows.reshape(rows, slots_max, HK, DH)
    value_heads = value_rows.reshape(rows, slots_max, HK, DH)
    scores = jnp.einsum(
        "nkgd,nskd->nkgs", query_heads, key_heads, preferred_element_type=jnp.float32
    ) * (1.0 / math.sqrt(DH))
    usable = jnp.arange(slots_max)[None, :] < lengths[:, None]
    scores = jnp.where(usable[:, None, None, :], scores, masked_score)
    block_max = jnp.max(scores, axis=-1)
    weights = jnp.exp(scores - block_max[..., None]).astype(jnp.bfloat16)
    block_sum = jnp.sum(weights.astype(jnp.float32), axis=-1)
    block_out = jnp.einsum(
        "nkgs,nskd->nkgd", weights, value_heads, preferred_element_type=jnp.float32
    )
    return block_out.reshape(rows, HQ, DH), block_max.reshape(rows, HQ), block_sum.reshape(rows, HQ)


def slot_table(owned_keys, device_key, capacity):
    entries = owned_keys.shape[0]
    alike_key = owned_keys[:, None] == owned_keys[None, :]
    position = jnp.arange(entries)
    earlier = position[None, :] < position[:, None]
    slot_rank = jnp.sum(alike_key & earlier, axis=1)
    matches = device_key[:, None, None] == owned_keys[None, None, :]
    placed = slot_rank[None, None, :] == jnp.arange(capacity)[None, :, None]
    return matches & placed


def merge_parts(part_out, part_max, part_sum, selection, suffix_out, suffix_max, suffix_sum):
    sources, slot_count = (part_max.shape[0], part_max.shape[1])
    rows = suffix_out.shape[0]
    masked = jnp.where(selection[..., None], part_max[:, :, None, :], masked_score)
    overall = jnp.maximum(jnp.max(masked, axis=(0, 1)), suffix_max)
    factor = jnp.where(selection[..., None], jnp.exp(masked - overall[None, None]), 0.0)
    out_heads = part_out.reshape(sources, slot_count, HQ, DH).astype(jnp.float32)
    suffix_factor = jnp.exp(suffix_max - overall)
    numerator = (
        jnp.einsum("scnh,schd->nhd", factor, out_heads, precision=lax.Precision.HIGHEST)
        + suffix_factor[..., None] * suffix_out
    )
    denominator = (
        jnp.einsum("scnh,sch->nh", factor, part_sum, precision=lax.Precision.HIGHEST)
        + suffix_factor * suffix_sum
    )
    return (numerator / denominator[..., None]).reshape(rows, HQ * DH).astype(jnp.bfloat16)


def local(
    queries,
    hidden_in,
    prefix_keys,
    prefix_values,
    suffix_keys,
    suffix_values,
    suffix_length,
    prefix_of,
    expert_index,
    gate_logits,
    norm_gain,
    gate_weight,
    up_weight,
    down_weight,
):
    devices = lax.axis_size("wide")
    rank_here = lax.axis_index("wide")
    rows, width = queries.shape
    half = devices // 2
    start_row = rank_here * rows
    siblings = [(i, i ^ 1) for i in range(devices)]
    alike = [[2 * i + c for i in range(half)] for c in range(2)]

    own_prefix = lax.dynamic_slice_in_dim(prefix_of[:, 0], start_row, rows, 0)
    selection = slot_table(own_prefix, jnp.arange(devices) // (devices // PREFIXES), CAPP)
    outgoing = jnp.einsum(
        "sci,id->scd", selection.astype(jnp.bfloat16), queries, preferred_element_type=jnp.float32
    ).astype(jnp.bfloat16)
    received = lax.all_to_all(outgoing, "wide", split_axis=0, concat_axis=0, tiled=True)
    suffix_out, suffix_max, suffix_sum = attend_suffix(
        queries, suffix_keys, suffix_values, suffix_length
    )
    part_out, part_max, part_sum = attend(
        received.reshape(devices * CAPP, width), prefix_keys, prefix_values
    )
    pieces = split_parts(part_max, 3) + split_parts(part_sum, 2)
    pad = jnp.zeros((devices * CAPP, STAT - 5 * HQ), jnp.bfloat16)
    packed = jnp.concatenate([part_out.astype(jnp.bfloat16)] + pieces + [pad], axis=1)
    back = lax.all_to_all(
        packed.reshape(devices, CAPP, width + STAT), "wide", split_axis=0, concat_axis=0, tiled=True
    )
    stats = back[:, :, width : width + 5 * HQ].astype(jnp.float32).reshape(devices, CAPP, 5, HQ)
    back_max = stats[:, :, 0] + stats[:, :, 1] + stats[:, :, 2]
    back_sum = stats[:, :, 3] + stats[:, :, 4]
    attended = merge_parts(
        back[:, :, :width], back_max, back_sum, selection, suffix_out, suffix_max, suffix_sum
    )
    stream = hidden_in.astype(jnp.float32) + attended.astype(jnp.float32)
    normed = (
        stream * lax.rsqrt(jnp.mean(stream * stream, axis=-1, keepdims=True) + 1e-05) * norm_gain
    ).astype(jnp.bfloat16)

    spread = jnp.broadcast_to(normed[None], (half, rows, width))
    near = lax.all_to_all(
        spread, "wide", split_axis=0, concat_axis=0, tiled=True, axis_index_groups=alike
    ).reshape(half * rows, width)
    far = lax.ppermute(near, "wide", siblings)
    piece = jnp.concatenate([near, far], axis=0)
    gate_part = jnp.dot(piece, gate_weight, preferred_element_type=jnp.float32)
    up_part = jnp.dot(piece, up_weight, preferred_element_type=jnp.float32)
    hidden_all = (jax.nn.silu(gate_part) * up_part).astype(jnp.bfloat16)
    partial = jnp.dot(hidden_all, down_weight, preferred_element_type=jnp.float32)
    swapped = lax.ppermute(partial[half * rows :], "wide", siblings)
    summed = (partial[: half * rows] + swapped).astype(jnp.bfloat16)
    parts = lax.all_to_all(
        summed.reshape(half, rows, width),
        "wide",
        split_axis=0,
        concat_axis=0,
        tiled=True,
        axis_index_groups=alike,
    )

    own_experts = lax.dynamic_slice_in_dim(expert_index, start_row, rows, 0)
    gates = jax.nn.softmax(lax.dynamic_slice_in_dim(gate_logits, start_row, rows, 0), axis=-1)
    expert_of = (2 * jnp.arange(half)) // (devices // EXPERTS)
    share = jnp.sum(
        gates[None] * (own_experts[None] == expert_of[:, None, None]).astype(jnp.float32), axis=2
    )
    mixture = jnp.sum(share[:, :, None] * parts.astype(jnp.float32), axis=0)
    return (attended, mixture.astype(jnp.bfloat16))


def solution(mesh):
    placed = (
        P(("groups", "wide"), None),
        P(("groups", "wide"), None),
        P(("groups", "wide"), None),
        P(("groups", "wide"), None),
        P(("groups", "wide"), None, None),
        P(("groups", "wide"), None, None),
        P(("groups", "wide")),
        P("groups", None),
        P("groups", None),
        P("groups", None),
        P(),
        P(None, "wide"),
        P(None, "wide"),
        P("wide", None),
    )
    return jax.shard_map(
        local,
        mesh=mesh,
        in_specs=placed,
        out_specs=(P(("groups", "wide"), None), P(("groups", "wide"), None)),
        check_vma=False,
    )
```

```python
import math

import jax
import jax.numpy as jnp
from jax import lax
from jax.experimental import pallas as pl
from jax.experimental.pallas import tpu as pltpu
from jax.sharding import PartitionSpec as P

HQ = 24
HK = 4
DH = 128
EXPERTS = 4
PREFIXES = 8
CAPP = 2
CAPE = 6

GROUP = HQ // HK
PIECE = GROUP * DH
STAT = 128
SLOT = 8
BLOCKS = CAPE * HK // SLOT
PER = CAPE // (SLOT - CAPE)

masked_score = -1e30
F32 = jnp.float32
BF16 = jnp.bfloat16
VMEM = pl.BlockSpec(memory_space=pltpu.VMEM)
SMEM = pl.BlockSpec(memory_space=pltpu.SMEM)
HBM = pl.BlockSpec(memory_space=pltpu.HBM)


def iotas(shape):
    return lax.broadcasted_iota(jnp.int32, shape, 0), lax.broadcasted_iota(jnp.int32, shape, 1)


def div(x, m):
    return jnp.right_shift(x, m.bit_length() - 1)


def mod(x, m):
    return jnp.bitwise_and(x, m - 1)


def one_hot(picked):
    return picked.astype(F32).astype(BF16)


def dot(a, b):
    return jnp.dot(a, b, preferred_element_type=F32)


def dot_t(a, b):
    return lax.dot_general(a, b, (((1,), (1,)), ((), ())), preferred_element_type=F32)


def by_row(index, values):
    out = jnp.zeros(index.shape, jnp.asarray(values[0]).dtype)
    for i, value in enumerate(values):
        out = jnp.where(index == i, value, out)
    return out


def prefix_slots(prefix_ref, start, rows):
    named = [prefix_ref[start + r] for r in range(rows)]
    ranks = []
    for r in range(rows):
        rank = jnp.int32(0)
        for q in range(r):
            rank += (named[q] == named[r]).astype(jnp.int32)
        ranks.append(rank)
    return named, ranks


def stack_pieces(x):
    return jnp.concatenate([x[:, k * PIECE : (k + 1) * PIECE] for k in range(HK)], axis=0)


def call(kernel, outs, ins, specs, flops=0, limit=24, scratch=(), moved=0, out_specs=None):
    return pl.pallas_call(
        kernel,
        out_shape=outs,
        in_specs=specs,
        out_specs=out_specs or jax.tree.map(lambda _: VMEM, outs),
        scratch_shapes=scratch,
        compiler_params=pltpu.CompilerParams(vmem_limit_bytes=limit * 1024 * 1024),
        cost_estimate=pl.CostEstimate(
            flops=flops, bytes_accessed=moved or 1 << 20, transcendentals=0
        ),
    )(*ins)


def send_queries(queries, prefix_of, devices):
    rows = queries.shape[0]
    holders = devices // PREFIXES

    def kernel(query_ref, prefix_ref, out_ref):
        start = lax.axis_index("wide") * rows
        named, ranks = prefix_slots(prefix_ref, start, rows)
        row, col = iotas((devices * HK * CAPP, HK * rows))
        device, k, c = div(row, HK * CAPP), mod(div(row, CAPP), HK), mod(row, CAPP)
        r = mod(col, rows)
        picked = (
            (k == div(col, rows)) & (div(device, holders) == by_row(r, named)) & (c == by_row(r, ranks))
        )
        pieces = stack_pieces(query_ref[...].astype(F32)).astype(BF16)
        out_ref[...] = dot(one_hot(picked), pieces).astype(BF16)

    return call(
        kernel,
        jax.ShapeDtypeStruct((devices * HK * CAPP, PIECE), BF16),
        (queries, prefix_of),
        [VMEM, SMEM],
    )


def softmax_block(query, keys, values, mask):
    scores = dot_t(query, keys) * (1.0 / math.sqrt(DH))
    if mask is not None:
        scores = jnp.where(mask, scores, masked_score)
    top = jnp.max(scores, axis=-1, keepdims=True)
    weights = jnp.exp(scores - top).astype(BF16)
    total = jnp.sum(weights.astype(F32), axis=-1, keepdims=True)
    return dot(weights, values), top, total


def heads_of(x):
    return jnp.concatenate([x[:, g * DH : (g + 1) * DH] for g in range(GROUP)], axis=0)


def own_suffix(queries, keys, values, lengths):
    rows = queries.shape[0]
    span = keys.shape[1]
    flat = (rows * span, keys.shape[2])

    def kernel(query_ref, key_ref, value_ref, length_ref, out_ref, stat_ref):
        row, col = iotas((rows, rows * span))
        owner = div(col, span)
        live = (owner == row) & (mod(col, span) < by_row(owner, [length_ref[r] for r in range(rows)]))
        mask = jnp.concatenate([live.astype(F32)] * GROUP, axis=0) > 0.5
        lane = iotas((rows, STAT))[1]
        query = query_ref[...].astype(F32)
        for k in range(HK):
            cols = pl.ds(k * DH, DH)
            own = pl.ds(k * rows, rows)
            out, top, total = softmax_block(
                heads_of(query[:, k * PIECE : (k + 1) * PIECE]).astype(BF16),
                key_ref[:, cols],
                value_ref[:, cols],
                mask,
            )
            stat = jnp.zeros((rows, STAT), F32)
            for g in range(GROUP):
                part = slice(g * rows, (g + 1) * rows)
                out_ref[own, pl.ds(g * DH, DH)] = out[part]
                stat = jnp.where(lane == g, top[part], stat)
                stat = jnp.where(lane == SLOT + g, total[part], stat)
            stat_ref[own, :] = stat

    return call(
        kernel,
        (
            jax.ShapeDtypeStruct((HK * rows, PIECE), F32),
            jax.ShapeDtypeStruct((HK * rows, STAT), F32),
        ),
        (queries, keys.reshape(flat), values.reshape(flat), lengths),
        [VMEM, VMEM, VMEM, SMEM],
        flops=1 << 29,
    )


def prefix_block(received, keys, values, devices):
    total_rows = devices * HK * CAPP
    slots = devices * CAPP

    def kernel(received_ref, key_ref, value_ref, out_ref):
        row, col = iotas((total_rows, total_rows))
        device, slot = mod(div(row, CAPP), devices), mod(row, CAPP)
        to_heads = (device * (HK * CAPP) + div(row, slots) * CAPP + slot) == col
        query = dot(one_hot(to_heads), received_ref[...])
        lane = iotas((slots, STAT))[1]
        field, head = div(lane, SLOT), mod(lane, SLOT)
        packed = []
        for k in range(HK):
            cols = pl.ds(k * DH, DH)
            out, top, total = softmax_block(
                heads_of(query[k * slots : (k + 1) * slots]).astype(BF16),
                key_ref[:, cols],
                value_ref[:, cols],
                None,
            )
            parts = [out[g * slots : (g + 1) * slots] for g in range(GROUP)]
            tops = by_row(head, [top[g * slots : (g + 1) * slots] for g in range(GROUP)])
            sums = by_row(head, [total[g * slots : (g + 1) * slots] for g in range(GROUP)])
            high = tops.astype(BF16).astype(F32)
            middle = (tops - high).astype(BF16).astype(F32)
            low = tops - high - middle
            sum_high = sums.astype(BF16).astype(F32)
            stat = by_row(field, [high, middle, low, sum_high, sums - sum_high])
            packed.append(jnp.concatenate(parts + [stat], axis=1))
        packed = jnp.concatenate(packed, axis=0).astype(BF16)
        device, k = div(row, HK * CAPP), mod(div(row, CAPP), HK)
        to_devices = (k * slots + device * CAPP + slot) == col
        out_ref[...] = dot(one_hot(to_devices), packed).astype(BF16)

    return call(
        kernel,
        jax.ShapeDtypeStruct((total_rows, PIECE + STAT), BF16),
        (received, keys, values),
        [VMEM, VMEM, VMEM],
    )


def routes(expert_index, gate_logits, devices, rows):
    half = devices // 2
    per_expert = half // EXPERTS

    def kernel(expert_ref, logit_ref, pack_ref, main_ref, tail_ref, gate_ref):
        start = lax.axis_index("wide") * rows
        named = [[expert_ref[j, start + r] for r in range(rows)] for j in range(2)]
        logits = [[logit_ref[j, start + r] for r in range(rows)] for j in range(2)]

        row, col = iotas((EXPERTS * SLOT, HK * rows))
        expert, i, k, r = div(row, SLOT), mod(row, SLOT), div(col, rows), mod(col, rows)
        has = (by_row(r, named[0]) == expert) | (by_row(r, named[1]) == expert)
        a, b = iotas((HK * rows, HK * rows))
        earlier = (div(a, rows) == div(b, rows)) & (mod(a, rows) < mod(b, rows))
        rank = dot(one_hot(has), one_hot(earlier)).astype(jnp.int32)
        for n in range(BLOCKS):
            slot = jnp.where(i < CAPE, i, (i - CAPE) * PER + n)
            piece = jnp.where(i < CAPE, n, HK - 1)
            pack_ref[n] = one_hot(has & (rank == slot) & (k == piece))

        row, col = iotas((2 * rows, half * SLOT))
        j, r = div(row, rows), mod(row, rows)
        expert, i = div(div(col, SLOT), per_expert), mod(col, SLOT)
        mine = jnp.where(j == 0, by_row(r, named[0]), by_row(r, named[1]))
        rank = jnp.zeros(row.shape, jnp.int32)
        for q in range(rows):
            same = (mine == named[0][q]) | (mine == named[1][q])
            rank += ((r > q) & same).astype(jnp.int32)
        here = expert == mine
        main_ref[...] = one_hot(here & (i == rank))
        for n in range(BLOCKS):
            spot = jnp.full(row.shape, -1, jnp.int32)
            for m in range(SLOT - CAPE):
                spot = jnp.where(rank == m * PER + n, CAPE + m, spot)
            tail_ref[n] = one_hot(here & (i == spot))

        row, _ = iotas((rows, STAT))
        first, second = by_row(row, logits[0]), by_row(row, logits[1])
        top = jnp.maximum(first, second)
        first, second = jnp.exp(first - top), jnp.exp(second - top)
        gate_ref[0] = first / (first + second)
        gate_ref[1] = second / (first + second)

    return call(
        kernel,
        (
            jax.ShapeDtypeStruct((BLOCKS, EXPERTS * SLOT, HK * rows), BF16),
            jax.ShapeDtypeStruct((2 * rows, half * SLOT), BF16),
            jax.ShapeDtypeStruct((BLOCKS, 2 * rows, half * SLOT), BF16),
            jax.ShapeDtypeStruct((2, rows, STAT), F32),
        ),
        (expert_index.T, gate_logits.T),
        [SMEM, SMEM],
        flops=1 << 29,
    )


def merge(back, suffix_out, suffix_stat, hidden_in, norm_gain, prefix_of, pack, devices):
    rows, width = hidden_in.shape
    holders = devices // PREFIXES
    half = devices // 2
    per_expert = half // EXPERTS

    def kernel(
        back_ref, suffix_ref, stat_ref, hidden_ref, gain_ref, prefix_ref, pack_ref, out_ref, sent_ref
    ):
        start = lax.axis_index("wide") * rows
        named, ranks = prefix_slots(prefix_ref, start, rows)
        firsts = [named[r] * (holders * HK * CAPP) + ranks[r] for r in range(rows)]
        row, col = iotas((HK * rows, back_ref.shape[0]))
        target = by_row(mod(row, rows), firsts) + div(row, rows) * CAPP
        stat = stat_ref[...]
        outs, tops, sums = [suffix_ref[...]], [stat[:, :SLOT]], [stat[:, SLOT : 2 * SLOT]]
        for h in range(holders):
            found = dot(one_hot(target + h * (HK * CAPP) == col), back_ref[...])
            stat = found[:, PIECE:]
            field = [stat[:, n * SLOT : (n + 1) * SLOT] for n in range(5)]
            outs.append(found[:, :PIECE])
            tops.append(field[0] + field[1] + field[2])
            sums.append(field[3] + field[4])
        overall = tops[0]
        for top in tops[1:]:
            overall = jnp.maximum(overall, top)
        factors = [jnp.exp(top - overall) for top in tops]
        scale = 1.0 / sum(f * s for f, s in zip(factors, sums))
        factors = [f * scale for f in factors]
        merged = []
        for g in range(GROUP):
            cols = slice(g * DH, (g + 1) * DH)
            merged.append(sum(o[:, cols] * f[:, g : g + 1] for o, f in zip(outs, factors)))
        attended = jnp.concatenate(merged, axis=1).astype(BF16).astype(F32)
        for k in range(HK):
            out_ref[:, pl.ds(k * PIECE, PIECE)] = attended[k * rows : (k + 1) * rows].astype(BF16)
        stream = stack_pieces(hidden_ref[...].astype(F32)) + attended
        squares = jnp.sum(stream * stream, axis=-1, keepdims=True)
        mean = sum(squares[k * rows : (k + 1) * rows] for k in range(HK)) * (1.0 / width)
        scale = jnp.concatenate([lax.rsqrt(mean + 1e-05)] * HK, axis=0)
        gain = jnp.concatenate(
            [
                jnp.broadcast_to(gain_ref[:, k * PIECE : (k + 1) * PIECE], (rows, PIECE))
                for k in range(HK)
            ],
            axis=0,
        )
        normed = (stream * scale * gain).astype(BF16)
        for n in range(BLOCKS):
            taken = dot(pack_ref[n], normed)
            for i in range(half):
                e = i // per_expert
                sent_ref[pl.ds(i * SLOT, SLOT), pl.ds(n * PIECE, PIECE)] = taken[
                    e * SLOT : (e + 1) * SLOT
                ].astype(BF16)

    return call(
        kernel,
        (
            jax.ShapeDtypeStruct((rows, width), BF16),
            jax.ShapeDtypeStruct((half * SLOT, BLOCKS * PIECE), BF16),
        ),
        (back, suffix_out, suffix_stat, hidden_in, norm_gain.reshape(1, width), prefix_of, pack),
        [VMEM, VMEM, VMEM, VMEM, VMEM, SMEM, VMEM],
    )


def cuts(total, step):
    return [(p, min(step, total - p)) for p in range(0, total, step)]


def experts(near, far, gate_weight, up_weight, down_weight):
    half = near.shape[0]
    units, width = down_weight.shape
    depth = 4
    unit_cuts = cuts(units, 512)
    out_cuts = cuts(width, 512)

    def kernel(
        near_ref, far_ref, gate_hbm, up_hbm, down_hbm, mine_ref, theirs_ref,
        gate_ref, up_ref, down_ref, rows_ref, hidden_ref, sems,
    ):
        copies = []
        for p, step in unit_cuts:
            copies.append((gate_hbm, gate_ref, pl.ds(p, step)))
            copies.append((up_hbm, up_ref, pl.ds(p, step)))
        for p, step in out_cuts:
            copies.append((down_hbm, down_ref, pl.ds(p, step)))

        def copy(n):
            source, target, cols = copies[n]
            return pltpu.make_async_copy(source.at[:, cols], target.at[:, cols], sems.at[n])

        for n in range(min(depth, len(copies))):
            copy(n).start()

        def arrive(n):
            copy(n).wait()
            if n + depth < len(copies):
                copy(n + depth).start()

        row, col = iotas((half, half))
        i, i_from = mod(row, SLOT), mod(col, SLOT)
        same = div(row, SLOT) == div(col, SLOT)
        for side, ref in enumerate((near_ref, far_ref)):
            own = pl.ds(side * half, half)
            tail = jnp.zeros((half, PIECE), F32)
            for n in range(BLOCKS):
                spot = jnp.full(row.shape, -1, jnp.int32)
                for m in range(SLOT - CAPE):
                    spot = jnp.where(i == m * PER + n, CAPE + m, spot)
                tail += dot(one_hot(same & (i_from == spot)), ref[:, n * PIECE : (n + 1) * PIECE])
            rows_ref[own, : BLOCKS * PIECE] = ref[...]
            rows_ref[own, BLOCKS * PIECE :] = tail.astype(BF16)
        for n, (p, step) in enumerate(unit_cuts):
            cols = pl.ds(p, step)
            arrive(2 * n)
            gate = dot(rows_ref[...], gate_ref[:, cols])
            arrive(2 * n + 1)
            up = dot(rows_ref[...], up_ref[:, cols])
            hidden_ref[:, cols] = (gate / (1.0 + jnp.exp(-gate)) * up).astype(BF16)
        for n, (p, step) in enumerate(out_cuts):
            cols = pl.ds(p, step)
            arrive(2 * len(unit_cuts) + n)
            part = dot(hidden_ref[...], down_ref[:, cols])
            mine_ref[:, cols] = part[:half]
            theirs_ref[:, cols] = part[half:]

    part = jax.ShapeDtypeStruct((half, width), F32)
    return call(
        kernel,
        (part, part),
        (near, far, gate_weight, up_weight, down_weight),
        [VMEM, VMEM, HBM, HBM, HBM],
        flops=12 * half * units * width,
        moved=6 * units * width,
        limit=56,
        scratch=[
            pltpu.VMEM(gate_weight.shape, BF16),
            pltpu.VMEM(up_weight.shape, BF16),
            pltpu.VMEM(down_weight.shape, BF16),
            pltpu.VMEM((2 * half, width), BF16),
            pltpu.VMEM((2 * half, units), BF16),
            pltpu.SemaphoreType.DMA((2 * len(unit_cuts) + len(out_cuts),)),
        ],
    )


def add_and_pack(mine, swapped):
    half, width = mine.shape

    def kernel(mine_ref, swapped_ref, out_ref):
        row, col = iotas((half, half))
        same = div(row, SLOT) == div(col, SLOT)
        i, i_from = mod(row, SLOT), mod(col, SLOT)
        keep = mod(iotas((half, PIECE))[0], SLOT) < CAPE
        last = pl.ds(BLOCKS * PIECE, PIECE)
        tail = (mine_ref[:, last] + swapped_ref[:, last]).astype(BF16)
        for n in range(BLOCKS):
            cols = pl.ds(n * PIECE, PIECE)
            moved = dot(one_hot(same & (i >= CAPE) & (i_from == (i - CAPE) * PER + n)), tail)
            out_ref[:, cols] = jnp.where(keep, mine_ref[:, cols] + swapped_ref[:, cols], moved).astype(BF16)

    return call(
        kernel,
        jax.ShapeDtypeStruct((half, BLOCKS * PIECE), BF16),
        (mine, swapped),
        [VMEM, VMEM],
    )


def mix(parts, main, tail, gates):
    rows = main.shape[0] // 2

    def kernel(part_ref, main_ref, tail_ref, gate_ref, out_ref):
        first, second = gate_ref[0][:, :1], gate_ref[1][:, :1]
        last = jnp.zeros((2 * rows, PIECE), F32)
        for n in range(BLOCKS):
            cols = pl.ds(n * PIECE, PIECE)
            found = dot(main_ref[...], part_ref[:, cols])
            out_ref[:, cols] = (found[:rows] * first + found[rows:] * second).astype(BF16)
            last += dot(tail_ref[n], part_ref[:, cols])
        cols = pl.ds(BLOCKS * PIECE, PIECE)
        out_ref[:, cols] = (last[:rows] * first + last[rows:] * second).astype(BF16)

    return call(
        kernel,
        jax.ShapeDtypeStruct((rows, HK * PIECE), BF16),
        (parts, main, tail, gates),
        [VMEM, VMEM, VMEM, VMEM],
    )


def exchange(x, groups=None):
    return lax.all_to_all(x, "wide", 0, 0, tiled=True, axis_index_groups=groups)


def local(
    queries,
    hidden_in,
    prefix_keys,
    prefix_values,
    suffix_keys,
    suffix_values,
    suffix_length,
    prefix_of,
    expert_index,
    gate_logits,
    norm_gain,
    gate_weight,
    up_weight,
    down_weight,
):
    devices = lax.axis_size("wide")
    rows = queries.shape[0]
    half = devices // 2
    siblings = [(i, i ^ 1) for i in range(devices)]
    alike = [[2 * i + c for i in range(half)] for c in range(2)]
    prefix_of = prefix_of[:, 0]

    received = exchange(send_queries(queries, prefix_of, devices))
    suffix_out, suffix_stat = own_suffix(queries, suffix_keys, suffix_values, suffix_length)
    pack, main, tail, gates = routes(expert_index, gate_logits, devices, rows)
    back = exchange(prefix_block(received, prefix_keys, prefix_values, devices))
    attended, sent = merge(
        back, suffix_out, suffix_stat, hidden_in, norm_gain, prefix_of, pack, devices
    )
    near = exchange(sent, alike)
    far = lax.ppermute(near, "wide", siblings)
    mine, theirs = experts(near, far, gate_weight, up_weight, down_weight)
    swapped = lax.ppermute(theirs, "wide", siblings)
    parts = exchange(add_and_pack(mine, swapped), alike)
    return attended, mix(parts, main, tail, gates)


def solution(mesh):
    placed = (
        P(("groups", "wide"), None),
        P(("groups", "wide"), None),
        P(("groups", "wide"), None),
        P(("groups", "wide"), None),
        P(("groups", "wide"), None, None),
        P(("groups", "wide"), None, None),
        P(("groups", "wide")),
        P("groups", None),
        P("groups", None),
        P("groups", None),
        P(),
        P(None, "wide"),
        P(None, "wide"),
        P("wide", None),
    )
    return jax.shard_map(
        local,
        mesh=mesh,
        in_specs=placed,
        out_specs=(P(("groups", "wide"), None), P(("groups", "wide"), None)),
        check_vma=False,
    )
```

```python
import math

import jax
import jax.numpy as jnp
from jax import lax
from jax.experimental import pallas as pl
from jax.experimental.pallas import tpu as pltpu
from jax.sharding import PartitionSpec as P

HQ = 24
HK = 4
DH = 128
EXPERTS = 4
PREFIXES = 8
CAPP = 2
CAPE = 6

GROUP = HQ // HK
PIECE = GROUP * DH
STAT = 128
SLOT = 8
BLOCKS = CAPE * HK // SLOT
PER = CAPE // (SLOT - CAPE)

masked_score = -1e30
F32 = jnp.float32
BF16 = jnp.bfloat16
VMEM = pl.BlockSpec(memory_space=pltpu.VMEM)
SMEM = pl.BlockSpec(memory_space=pltpu.SMEM)
HBM = pl.BlockSpec(memory_space=pltpu.HBM)


def iotas(shape):
    return lax.broadcasted_iota(jnp.int32, shape, 0), lax.broadcasted_iota(jnp.int32, shape, 1)


def div(x, m):
    return jnp.right_shift(x, m.bit_length() - 1)


def mod(x, m):
    return jnp.bitwise_and(x, m - 1)


def one_hot(picked):
    return picked.astype(F32).astype(BF16)


def dot(a, b):
    return jnp.dot(a, b, preferred_element_type=F32)


def dot_t(a, b):
    return lax.dot_general(a, b, (((1,), (1,)), ((), ())), preferred_element_type=F32)


def by_row(index, values):
    out = jnp.zeros(index.shape, jnp.asarray(values[0]).dtype)
    for i, value in enumerate(values):
        out = jnp.where(index == i, value, out)
    return out


def prefix_slots(prefix_ref, start, rows):
    named = [prefix_ref[start + r] for r in range(rows)]
    ranks = []
    for r in range(rows):
        rank = jnp.int32(0)
        for q in range(r):
            rank += (named[q] == named[r]).astype(jnp.int32)
        ranks.append(rank)
    return named, ranks


def stack_pieces(x):
    return jnp.concatenate([x[:, k * PIECE : (k + 1) * PIECE] for k in range(HK)], axis=0)


def call(kernel, outs, ins, specs, flops=0, limit=24, scratch=(), moved=0, out_specs=None):
    ins = [pltpu.with_memory_space_constraint(x, pltpu.HBM) if s is HBM else x for x, s in zip(ins, specs)]
    return pl.pallas_call(
        kernel,
        out_shape=outs,
        in_specs=specs,
        out_specs=out_specs or jax.tree.map(lambda _: VMEM, outs),
        scratch_shapes=scratch,
        compiler_params=pltpu.CompilerParams(vmem_limit_bytes=limit * 1024 * 1024),
        cost_estimate=pl.CostEstimate(
            flops=flops, bytes_accessed=moved or 1 << 20, transcendentals=0
        ),
    )(*ins)


def fetch(pairs, sems):
    copies = [pltpu.make_async_copy(s, t, sems.at[n]) for n, (s, t) in enumerate(pairs)]
    for copy in copies:
        copy.start()
    return copies


def send_queries(queries, prefix_of, devices):
    rows = queries.shape[0]
    holders = devices // PREFIXES

    def kernel(query_hbm, prefix_hbm, out_ref, query_ref, prefix_ref, sems):
        copies = fetch([(prefix_hbm, prefix_ref), (query_hbm, query_ref)], sems)
        row, col = iotas((devices * HK * CAPP, HK * rows))
        device, k, c = div(row, HK * CAPP), mod(div(row, CAPP), HK), mod(row, CAPP)
        r = mod(col, rows)
        copies[0].wait()
        start = lax.axis_index("wide") * rows
        named, ranks = prefix_slots(prefix_ref, start, rows)
        picked = (
            (k == div(col, rows)) & (div(device, holders) == by_row(r, named)) & (c == by_row(r, ranks))
        )
        copies[1].wait()
        pieces = stack_pieces(query_ref[...].astype(F32)).astype(BF16)
        out_ref[...] = dot(one_hot(picked), pieces).astype(BF16)

    return call(
        kernel,
        jax.ShapeDtypeStruct((devices * HK * CAPP, PIECE), BF16),
        (queries, prefix_of),
        [HBM, HBM],
        scratch=[
            pltpu.VMEM(queries.shape, BF16),
            pltpu.SMEM(prefix_of.shape, jnp.int32),
            pltpu.SemaphoreType.DMA((2,)),
        ],
        limit=4,
    )


def softmax_block(query, keys, values, mask):
    scores = dot_t(query, keys) * (1.0 / math.sqrt(DH))
    if mask is not None:
        scores = jnp.where(mask, scores, masked_score)
    top = jnp.max(scores, axis=-1, keepdims=True)
    weights = jnp.exp(scores - top).astype(BF16)
    total = jnp.sum(weights.astype(F32), axis=-1, keepdims=True)
    return dot(weights, values), top, total


def heads_of(x):
    return jnp.concatenate([x[:, g * DH : (g + 1) * DH] for g in range(GROUP)], axis=0)


def own_suffix(query, key_ref, value_ref, lengths, out_ref, stat_ref):
    rows = query.shape[0]
    span = key_ref.shape[0] // rows
    row, col = iotas((rows, rows * span))
    owner = div(col, span)
    live = (owner == row) & (mod(col, span) < by_row(owner, lengths))
    mask = jnp.concatenate([live.astype(F32)] * GROUP, axis=0) > 0.5
    lane = iotas((rows, STAT))[1]
    for k in range(HK):
        cols = pl.ds(k * DH, DH)
        own = pl.ds(k * rows, rows)
        out, top, total = softmax_block(
            heads_of(query[:, k * PIECE : (k + 1) * PIECE]).astype(BF16),
            key_ref[:, cols],
            value_ref[:, cols],
            mask,
        )
        stat = jnp.zeros((rows, STAT), F32)
        for g in range(GROUP):
            part = slice(g * rows, (g + 1) * rows)
            out_ref[own, pl.ds(g * DH, DH)] = out[part]
            stat = jnp.where(lane == g, top[part], stat)
            stat = jnp.where(lane == SLOT + g, total[part], stat)
        stat_ref[own, :] = stat


def prefix_block(received, keys, values, devices):
    total_rows = devices * HK * CAPP
    slots = devices * CAPP

    def kernel(received_ref, key_ref, value_ref, out_ref):
        row, col = iotas((total_rows, total_rows))
        device, slot = mod(div(row, CAPP), devices), mod(row, CAPP)
        to_heads = (device * (HK * CAPP) + div(row, slots) * CAPP + slot) == col
        query = dot(one_hot(to_heads), received_ref[...])
        lane = iotas((slots, STAT))[1]
        field, head = div(lane, SLOT), mod(lane, SLOT)
        packed = []
        for k in range(HK):
            cols = pl.ds(k * DH, DH)
            out, top, total = softmax_block(
                heads_of(query[k * slots : (k + 1) * slots]).astype(BF16),
                key_ref[:, cols],
                value_ref[:, cols],
                None,
            )
            parts = [out[g * slots : (g + 1) * slots] for g in range(GROUP)]
            tops = by_row(head, [top[g * slots : (g + 1) * slots] for g in range(GROUP)])
            sums = by_row(head, [total[g * slots : (g + 1) * slots] for g in range(GROUP)])
            high = tops.astype(BF16).astype(F32)
            middle = (tops - high).astype(BF16).astype(F32)
            low = tops - high - middle
            sum_high = sums.astype(BF16).astype(F32)
            stat = by_row(field, [high, middle, low, sum_high, sums - sum_high])
            packed.append(jnp.concatenate(parts + [stat], axis=1))
        packed = jnp.concatenate(packed, axis=0).astype(BF16)
        device, k = div(row, HK * CAPP), mod(div(row, CAPP), HK)
        to_devices = (k * slots + device * CAPP + slot) == col
        out_ref[...] = dot(one_hot(to_devices), packed).astype(BF16)

    return call(
        kernel,
        jax.ShapeDtypeStruct((total_rows, PIECE + STAT), BF16),
        (received, keys, values),
        [VMEM, VMEM, VMEM],
        limit=8,
    )


def routes(named, logits, half, pack_ref, main_ref, tail_ref, gate_ref):
    rows = len(named[0])
    per_expert = half // EXPERTS
    row, col = iotas((EXPERTS * SLOT, HK * rows))
    expert, i, k, r = div(row, SLOT), mod(row, SLOT), div(col, rows), mod(col, rows)
    has = (by_row(r, named[0]) == expert) | (by_row(r, named[1]) == expert)
    a, b = iotas((HK * rows, HK * rows))
    earlier = (div(a, rows) == div(b, rows)) & (mod(a, rows) < mod(b, rows))
    rank = dot(one_hot(has), one_hot(earlier)).astype(jnp.int32)
    for n in range(BLOCKS):
        slot = jnp.where(i < CAPE, i, (i - CAPE) * PER + n)
        piece = jnp.where(i < CAPE, n, HK - 1)
        pack_ref[n] = one_hot(has & (rank == slot) & (k == piece))

    row, col = iotas((2 * rows, half * SLOT))
    j, r = div(row, rows), mod(row, rows)
    expert, i = div(div(col, SLOT), per_expert), mod(col, SLOT)
    mine = jnp.where(j == 0, by_row(r, named[0]), by_row(r, named[1]))
    rank = jnp.zeros(row.shape, jnp.int32)
    for q in range(rows):
        same = (mine == named[0][q]) | (mine == named[1][q])
        rank += ((r > q) & same).astype(jnp.int32)
    here = expert == mine
    main_ref[...] = one_hot(here & (i == rank))
    for n in range(BLOCKS):
        spot = jnp.full(row.shape, -1, jnp.int32)
        for m in range(SLOT - CAPE):
            spot = jnp.where(rank == m * PER + n, CAPE + m, spot)
        tail_ref[n] = one_hot(here & (i == spot))

    row, _ = iotas((rows, STAT))
    first, second = by_row(row, logits[0]), by_row(row, logits[1])
    top = jnp.maximum(first, second)
    first, second = jnp.exp(first - top), jnp.exp(second - top)
    gate_ref[0] = first / (first + second)
    gate_ref[1] = second / (first + second)


def prepare(
    queries, suffix_keys, suffix_values, lengths, prefix_of, expert_index, gate_logits,
    keys, values, hidden_in, norm_gain, devices,
):
    rows = queries.shape[0]
    half = devices // 2
    holders = devices // PREFIXES
    flat = (rows * suffix_keys.shape[1], suffix_keys.shape[2])
    gain = norm_gain.reshape(1, norm_gain.shape[0])
    expert_index, gate_logits = expert_index.T, gate_logits.T

    def kernel(
        query_hbm, skey_hbm, svalue_hbm, length_hbm, prefix_hbm, expert_hbm, logit_hbm,
        key_hbm, value_hbm, hidden_hbm, gain_hbm,
        suffix_ref, stat_ref, pack_ref, main_ref, tail_ref, gate_ref, find_ref,
        key_ref, value_ref, hidden_ref, gain_ref,
        query_ref, skey_ref, svalue_ref, length_ref, prefix_ref, expert_ref, logit_ref, sems,
    ):
        copies = fetch(
            [
                (expert_hbm, expert_ref), (logit_hbm, logit_ref), (prefix_hbm, prefix_ref),
                (length_hbm, length_ref), (query_hbm, query_ref), (skey_hbm, skey_ref),
                (svalue_hbm, svalue_ref), (key_hbm, key_ref), (value_hbm, value_ref),
                (hidden_hbm, hidden_ref), (gain_hbm, gain_ref),
            ],
            sems,
        )
        start = lax.axis_index("wide") * rows
        for copy in copies[:3]:
            copy.wait()
        named = [[expert_ref[j, start + r] for r in range(rows)] for j in range(2)]
        logits = [[logit_ref[j, start + r] for r in range(rows)] for j in range(2)]
        routes(named, logits, half, pack_ref, main_ref, tail_ref, gate_ref)

        named, ranks = prefix_slots(prefix_ref, start, rows)
        firsts = [named[r] * (holders * HK * CAPP) + ranks[r] for r in range(rows)]
        row, col = iotas((HK * rows, devices * HK * CAPP))
        target = by_row(mod(row, rows), firsts) + div(row, rows) * CAPP
        for h in range(holders):
            find_ref[h] = one_hot(target + h * (HK * CAPP) == col)

        for copy in copies[3:7]:
            copy.wait()
        lengths = [length_ref[r] for r in range(rows)]
        own_suffix(query_ref[...].astype(F32), skey_ref, svalue_ref, lengths, suffix_ref, stat_ref)
        for copy in copies[7:]:
            copy.wait()

    shape = jax.ShapeDtypeStruct
    return call(
        kernel,
        (
            shape((HK * rows, PIECE), F32),
            shape((HK * rows, STAT), F32),
            shape((BLOCKS, EXPERTS * SLOT, HK * rows), BF16),
            shape((2 * rows, half * SLOT), BF16),
            shape((BLOCKS, 2 * rows, half * SLOT), BF16),
            shape((2, rows, STAT), F32),
            shape((holders, HK * rows, devices * HK * CAPP), BF16),
            shape(keys.shape, BF16),
            shape(values.shape, BF16),
            shape(hidden_in.shape, BF16),
            shape(gain.shape, F32),
        ),
        (
            queries, suffix_keys.reshape(flat), suffix_values.reshape(flat), lengths, prefix_of,
            expert_index, gate_logits, keys, values, hidden_in, gain,
        ),
        [HBM] * 11,
        flops=1 << 31,
        scratch=[
            pltpu.VMEM(queries.shape, BF16),
            pltpu.VMEM(flat, BF16),
            pltpu.VMEM(flat, BF16),
            pltpu.SMEM(lengths.shape, jnp.int32),
            pltpu.SMEM(prefix_of.shape, jnp.int32),
            pltpu.SMEM(expert_index.shape, jnp.int32),
            pltpu.SMEM(gate_logits.shape, F32),
            pltpu.SemaphoreType.DMA((11,)),
        ],
        limit=8,
    )


def merge(back, suffix_out, suffix_stat, hidden_in, gain, find, pack, devices):
    rows, width = hidden_in.shape
    half = devices // 2
    per_expert = half // EXPERTS

    def kernel(
        back_ref, suffix_ref, stat_ref, hidden_ref, gain_ref, find_ref, pack_ref, out_ref, sent_ref
    ):
        stat = stat_ref[...]
        outs, tops, sums = [suffix_ref[...]], [stat[:, :SLOT]], [stat[:, SLOT : 2 * SLOT]]
        for h in range(find_ref.shape[0]):
            found = dot(find_ref[h], back_ref[...])
            stat = found[:, PIECE:]
            field = [stat[:, n * SLOT : (n + 1) * SLOT] for n in range(5)]
            outs.append(found[:, :PIECE])
            tops.append(field[0] + field[1] + field[2])
            sums.append(field[3] + field[4])
        overall = tops[0]
        for top in tops[1:]:
            overall = jnp.maximum(overall, top)
        factors = [jnp.exp(top - overall) for top in tops]
        scale = 1.0 / sum(f * s for f, s in zip(factors, sums))
        factors = [f * scale for f in factors]
        merged = []
        for g in range(GROUP):
            cols = slice(g * DH, (g + 1) * DH)
            merged.append(sum(o[:, cols] * f[:, g : g + 1] for o, f in zip(outs, factors)))
        attended = jnp.concatenate(merged, axis=1).astype(BF16).astype(F32)
        for k in range(HK):
            out_ref[:, pl.ds(k * PIECE, PIECE)] = attended[k * rows : (k + 1) * rows].astype(BF16)
        stream = stack_pieces(hidden_ref[...].astype(F32)) + attended
        squares = jnp.sum(stream * stream, axis=-1, keepdims=True)
        mean = sum(squares[k * rows : (k + 1) * rows] for k in range(HK)) * (1.0 / width)
        scale = jnp.concatenate([lax.rsqrt(mean + 1e-05)] * HK, axis=0)
        gain = jnp.concatenate(
            [
                jnp.broadcast_to(gain_ref[:, k * PIECE : (k + 1) * PIECE], (rows, PIECE))
                for k in range(HK)
            ],
            axis=0,
        )
        normed = (stream * scale * gain).astype(BF16)
        for n in range(BLOCKS):
            taken = dot(pack_ref[n], normed)
            for i in range(half):
                e = i // per_expert
                sent_ref[pl.ds(i * SLOT, SLOT), pl.ds(n * PIECE, PIECE)] = taken[
                    e * SLOT : (e + 1) * SLOT
                ].astype(BF16)

    return call(
        kernel,
        (
            jax.ShapeDtypeStruct((rows, width), BF16),
            jax.ShapeDtypeStruct((half * SLOT, BLOCKS * PIECE), BF16),
        ),
        (back, suffix_out, suffix_stat, hidden_in, gain, find, pack),
        [VMEM] * 7,
        limit=8,
    )


def cuts(total, step):
    return [(p, min(step, total - p)) for p in range(0, total, step)]


def experts(near, far, gate_weight, up_weight, down_weight):
    half = near.shape[0]
    units, width = down_weight.shape
    depth = 4
    unit_cuts = cuts(units, 512)
    out_cuts = cuts(width, 512)

    def kernel(
        near_ref, far_ref, gate_hbm, up_hbm, down_hbm, mine_ref, theirs_ref,
        gate_ref, up_ref, down_ref, rows_ref, hidden_ref, sems,
    ):
        copies = []
        for p, step in unit_cuts:
            copies.append((gate_hbm, gate_ref, pl.ds(p, step)))
            copies.append((up_hbm, up_ref, pl.ds(p, step)))
        for p, step in out_cuts:
            copies.append((down_hbm, down_ref, pl.ds(p, step)))

        def copy(n):
            source, target, cols = copies[n]
            return pltpu.make_async_copy(source.at[:, cols], target.at[:, cols], sems.at[n])

        for n in range(min(depth, len(copies))):
            copy(n).start()

        def arrive(n):
            copy(n).wait()
            if n + depth < len(copies):
                copy(n + depth).start()

        row, col = iotas((half, half))
        i, i_from = mod(row, SLOT), mod(col, SLOT)
        same = div(row, SLOT) == div(col, SLOT)
        for side, ref in enumerate((near_ref, far_ref)):
            own = pl.ds(side * half, half)
            tail = jnp.zeros((half, PIECE), F32)
            for n in range(BLOCKS):
                spot = jnp.full(row.shape, -1, jnp.int32)
                for m in range(SLOT - CAPE):
                    spot = jnp.where(i == m * PER + n, CAPE + m, spot)
                tail += dot(one_hot(same & (i_from == spot)), ref[:, n * PIECE : (n + 1) * PIECE])
            rows_ref[own, : BLOCKS * PIECE] = ref[...]
            rows_ref[own, BLOCKS * PIECE :] = tail.astype(BF16)
        for n, (p, step) in enumerate(unit_cuts):
            cols = pl.ds(p, step)
            arrive(2 * n)
            gate = dot(rows_ref[...], gate_ref[:, cols])
            arrive(2 * n + 1)
            up = dot(rows_ref[...], up_ref[:, cols])
            hidden_ref[:, cols] = (gate / (1.0 + jnp.exp(-gate)) * up).astype(BF16)
        for n, (p, step) in enumerate(out_cuts):
            cols = pl.ds(p, step)
            arrive(2 * len(unit_cuts) + n)
            part = dot(hidden_ref[...], down_ref[:, cols])
            mine_ref[:, cols] = part[:half]
            theirs_ref[:, cols] = part[half:]

    part = jax.ShapeDtypeStruct((half, width), F32)
    return call(
        kernel,
        (part, part),
        (near, far, gate_weight, up_weight, down_weight),
        [VMEM, VMEM, HBM, HBM, HBM],
        flops=12 * half * units * width,
        moved=6 * units * width,
        limit=42,
        scratch=[
            pltpu.VMEM(gate_weight.shape, BF16),
            pltpu.VMEM(up_weight.shape, BF16),
            pltpu.VMEM(down_weight.shape, BF16),
            pltpu.VMEM((2 * half, width), BF16),
            pltpu.VMEM((2 * half, units), BF16),
            pltpu.SemaphoreType.DMA((2 * len(unit_cuts) + len(out_cuts),)),
        ],
    )


def add_and_pack(mine, swapped):
    half, width = mine.shape

    def kernel(mine_ref, swapped_ref, out_ref):
        row, col = iotas((half, half))
        same = div(row, SLOT) == div(col, SLOT)
        i, i_from = mod(row, SLOT), mod(col, SLOT)
        keep = mod(iotas((half, PIECE))[0], SLOT) < CAPE
        last = pl.ds(BLOCKS * PIECE, PIECE)
        tail = (mine_ref[:, last] + swapped_ref[:, last]).astype(BF16)
        for n in range(BLOCKS):
            cols = pl.ds(n * PIECE, PIECE)
            moved = dot(one_hot(same & (i >= CAPE) & (i_from == (i - CAPE) * PER + n)), tail)
            out_ref[:, cols] = jnp.where(keep, mine_ref[:, cols] + swapped_ref[:, cols], moved).astype(BF16)

    return call(
        kernel,
        jax.ShapeDtypeStruct((half, BLOCKS * PIECE), BF16),
        (mine, swapped),
        [VMEM, VMEM],
    )


def mix(parts, main, tail, gates):
    rows = main.shape[0] // 2

    def kernel(part_ref, main_ref, tail_ref, gate_ref, out_ref):
        first, second = gate_ref[0][:, :1], gate_ref[1][:, :1]
        last = jnp.zeros((2 * rows, PIECE), F32)
        for n in range(BLOCKS):
            cols = pl.ds(n * PIECE, PIECE)
            found = dot(main_ref[...], part_ref[:, cols])
            out_ref[:, cols] = (found[:rows] * first + found[rows:] * second).astype(BF16)
            last += dot(tail_ref[n], part_ref[:, cols])
        cols = pl.ds(BLOCKS * PIECE, PIECE)
        out_ref[:, cols] = (last[:rows] * first + last[rows:] * second).astype(BF16)

    return call(
        kernel,
        jax.ShapeDtypeStruct((rows, HK * PIECE), BF16),
        (parts, main, tail, gates),
        [VMEM, VMEM, VMEM, VMEM],
    )


def exchange(x, groups=None):
    return lax.all_to_all(x, "wide", 0, 0, tiled=True, axis_index_groups=groups)


def local(
    queries,
    hidden_in,
    prefix_keys,
    prefix_values,
    suffix_keys,
    suffix_values,
    suffix_length,
    prefix_of,
    expert_index,
    gate_logits,
    norm_gain,
    gate_weight,
    up_weight,
    down_weight,
):
    devices = lax.axis_size("wide")
    rows = queries.shape[0]
    half = devices // 2
    siblings = [(i, i ^ 1) for i in range(devices)]
    alike = [[2 * i + c for i in range(half)] for c in range(2)]
    prefix_of = prefix_of[:, 0]

    outgoing = send_queries(queries, prefix_of, devices)
    outgoing, suffix_length = lax.optimization_barrier((outgoing, suffix_length))
    received = exchange(outgoing)
    suffix_out, suffix_stat, pack, main, tail, gates, find, keys, values, hidden, gain = prepare(
        queries, suffix_keys, suffix_values, suffix_length, prefix_of, expert_index, gate_logits,
        prefix_keys, prefix_values, hidden_in, norm_gain, devices,
    )
    back = exchange(prefix_block(received, keys, values, devices))
    attended, sent = merge(back, suffix_out, suffix_stat, hidden, gain, find, pack, devices)
    near = exchange(sent, alike)
    far = lax.ppermute(near, "wide", siblings)
    mine, theirs = experts(near, far, gate_weight, up_weight, down_weight)
    swapped = lax.ppermute(theirs, "wide", siblings)
    parts = exchange(add_and_pack(mine, swapped), alike)
    return attended, mix(parts, main, tail, gates)


def solution(mesh):
    placed = (
        P(("groups", "wide"), None),
        P(("groups", "wide"), None),
        P(("groups", "wide"), None),
        P(("groups", "wide"), None),
        P(("groups", "wide"), None, None),
        P(("groups", "wide"), None, None),
        P(("groups", "wide")),
        P("groups", None),
        P("groups", None),
        P("groups", None),
        P(),
        P(None, "wide"),
        P(None, "wide"),
        P("wide", None),
    )
    return jax.shard_map(
        local,
        mesh=mesh,
        in_specs=placed,
        out_specs=(P(("groups", "wide"), None), P(("groups", "wide"), None)),
        check_vma=False,
    )
```

```python
import functools
import math

import jax
import jax.numpy as jnp
from jax import lax
from jax.experimental import pallas as pl
from jax.experimental.pallas import tpu as pltpu
from jax.sharding import PartitionSpec as P

HQ = 24
HK = 4
DH = 128
EXPERTS = 4
PREFIXES = 8
CAPP = 2
CAPE = 6

GROUP = HQ // HK
PIECE = GROUP * DH
STAT = 128
SLOT = 8
BLOCKS = CAPE * HK // SLOT
PER = CAPE // (SLOT - CAPE)

masked_score = -1e30
F32 = jnp.float32
BF16 = jnp.bfloat16
VMEM = pl.BlockSpec(memory_space=pltpu.VMEM)
SMEM = pl.BlockSpec(memory_space=pltpu.SMEM)
HBM = pl.BlockSpec(memory_space=pltpu.HBM)


def iotas(shape):
    return lax.broadcasted_iota(jnp.int32, shape, 0), lax.broadcasted_iota(jnp.int32, shape, 1)


def div(x, m):
    return jnp.right_shift(x, m.bit_length() - 1)


def mod(x, m):
    return jnp.bitwise_and(x, m - 1)


def one_hot(picked):
    return picked.astype(F32).astype(BF16)


def dot(a, b):
    return jnp.dot(a, b, preferred_element_type=F32)


def dot_t(a, b):
    return lax.dot_general(a, b, (((1,), (1,)), ((), ())), preferred_element_type=F32)


def by_row(index, values):
    out = jnp.zeros(index.shape, jnp.asarray(values[0]).dtype)
    for i, value in enumerate(values):
        out = jnp.where(index == i, value, out)
    return out


def prefix_slots(prefix_ref, start, rows):
    named = [prefix_ref[start + r] for r in range(rows)]
    ranks = []
    for r in range(rows):
        rank = jnp.int32(0)
        for q in range(r):
            rank += (named[q] == named[r]).astype(jnp.int32)
        ranks.append(rank)
    return named, ranks


def stack_pieces(x):
    return jnp.concatenate([x[:, k * PIECE : (k + 1) * PIECE] for k in range(HK)], axis=0)


def call(kernel, outs, ins, specs, flops=0, limit=24, scratch=(), moved=0, out_specs=None):
    ins = [pltpu.with_memory_space_constraint(x, pltpu.HBM) if s is HBM else x for x, s in zip(ins, specs)]
    return pl.pallas_call(
        kernel,
        out_shape=outs,
        in_specs=specs,
        out_specs=out_specs or jax.tree.map(lambda _: VMEM, outs),
        scratch_shapes=scratch,
        compiler_params=pltpu.CompilerParams(vmem_limit_bytes=limit * 1024 * 1024),
        cost_estimate=pl.CostEstimate(
            flops=flops, bytes_accessed=moved or 1 << 20, transcendentals=0
        ),
    )(*ins)


def fetch(pairs, sems):
    copies = [pltpu.make_async_copy(s, t, sems.at[n]) for n, (s, t) in enumerate(pairs)]
    for copy in copies:
        copy.start()
    return copies


def send_queries(queries, prefix_of, devices):
    rows = queries.shape[0]
    chips = devices // 2
    holders = devices // 2 // PREFIXES

    def kernel(query_hbm, prefix_hbm, out_ref, query_ref, prefix_ref, sems):
        copies = fetch([(prefix_hbm, prefix_ref), (query_hbm, query_ref)], sems)
        row, col = iotas((chips * HK * CAPP, HK * rows))
        chip, k, c = div(row, HK * CAPP), mod(div(row, CAPP), HK), mod(row, CAPP)
        r = mod(col, rows)
        copies[0].wait()
        start = lax.axis_index("wide") * rows
        named, ranks = prefix_slots(prefix_ref, start, rows)
        picked = (
            (k == div(col, rows)) & (div(chip, holders) == by_row(r, named)) & (c == by_row(r, ranks))
        )
        copies[1].wait()
        pieces = stack_pieces(query_ref[...].astype(F32)).astype(BF16)
        out_ref[...] = dot(one_hot(picked), pieces).astype(BF16)

    return call(
        kernel,
        pltpu.VMEM((chips * HK * CAPP, PIECE), BF16),
        (queries, prefix_of),
        [HBM, HBM],
        scratch=[
            pltpu.VMEM(queries.shape, BF16),
            pltpu.SMEM(prefix_of.shape, jnp.int32),
            pltpu.SemaphoreType.DMA((2,)),
        ],
        limit=4,
        out_specs=VMEM,
    )


def softmax_block(query, keys, values, mask):
    scores = dot_t(query, keys) * (1.0 / math.sqrt(DH))
    if mask is not None:
        scores = jnp.where(mask, scores, masked_score)
    top = jnp.max(scores, axis=-1, keepdims=True)
    weights = jnp.exp(scores - top).astype(BF16)
    total = jnp.sum(weights.astype(F32), axis=-1, keepdims=True)
    return dot(weights, values), top, total


def heads_of(x):
    return jnp.concatenate([x[:, g * DH : (g + 1) * DH] for g in range(GROUP)], axis=0)


def own_suffix(query, key_ref, value_ref, lengths, out_ref, stat_ref):
    rows = query.shape[0]
    span = key_ref.shape[0] // rows
    row, col = iotas((rows, rows * span))
    owner = div(col, span)
    live = (owner == row) & (mod(col, span) < by_row(owner, lengths))
    mask = jnp.concatenate([live.astype(F32)] * GROUP, axis=0) > 0.5
    lane = iotas((rows, STAT))[1]
    for k in range(HK):
        cols = pl.ds(k * DH, DH)
        own = pl.ds(k * rows, rows)
        out, top, total = softmax_block(
            heads_of(query[:, k * PIECE : (k + 1) * PIECE]).astype(BF16),
            key_ref[:, cols],
            value_ref[:, cols],
            mask,
        )
        stat = jnp.zeros((rows, STAT), F32)
        for g in range(GROUP):
            part = slice(g * rows, (g + 1) * rows)
            out_ref[own, pl.ds(g * DH, DH)] = out[part]
            stat = jnp.where(lane == g, top[part], stat)
            stat = jnp.where(lane == SLOT + g, total[part], stat)
        stat_ref[own, :] = stat


def stats_of(field, head, tops, sums):
    return by_row(field, [by_row(head, tops), by_row(head, sums)])


def prefix_block(near, far, keys, values):
    side_rows = near.shape[0]
    total_rows = 2 * side_rows
    slots = total_rows // HK
    half = slots // 2

    def kernel(near_ref, far_ref, key_ref, value_ref, kept_ref, given_ref):
        row, col = iotas((total_rows, side_rows))
        k, slot = div(row, slots), mod(row, slots)
        side, slot = div(slot, half), mod(slot, half)
        source = div(slot, CAPP) * (HK * CAPP) + k * CAPP + mod(slot, CAPP)
        query = dot(one_hot((side == 0) & (source == col)), near_ref[...]) + dot(
            one_hot((side == 1) & (source == col)), far_ref[...]
        )
        lane = iotas((slots, STAT))[1]
        field, head = div(lane, SLOT), mod(lane, SLOT)
        for k in range(HK):
            cols = pl.ds(k * DH, DH)
            out, top, total = softmax_block(
                heads_of(query[k * slots : (k + 1) * slots]).astype(BF16),
                key_ref[:, cols],
                value_ref[:, cols],
                None,
            )
            tops = [top[g * slots : (g + 1) * slots] for g in range(GROUP)]
            sums = [total[g * slots : (g + 1) * slots] for g in range(GROUP)]
            stat = stats_of(field, head, tops, sums)
            own = pl.ds(k * half, half)
            for side, ref in enumerate((kept_ref, given_ref)):
                for g in range(GROUP):
                    first = g * slots + side * half
                    ref[own, pl.ds(g * DH, DH)] = out[first : first + half]
                ref[own, pl.ds(PIECE, STAT)] = stat[side * half : (side + 1) * half]

    part = jax.ShapeDtypeStruct((side_rows, PIECE + STAT), F32)
    return call(
        kernel,
        (part, part),
        (near, far, keys, values),
        [VMEM] * 4,
        limit=8,
    )


def join_blocks(kept, swapped):
    side_rows = kept.shape[0]
    slots = side_rows // HK

    def kernel(kept_ref, swapped_ref, out_ref):
        stat = [ref[:, PIECE:] for ref in (kept_ref, swapped_ref)]
        tops, sums = [s[:, :SLOT] for s in stat], [s[:, SLOT : 2 * SLOT] for s in stat]
        top = jnp.maximum(*tops)
        factors = [jnp.exp(t - top) for t in tops]
        total = factors[0] * sums[0] + factors[1] * sums[1]
        parts = []
        for g in range(GROUP):
            cols = pl.ds(g * DH, DH)
            parts.append(
                kept_ref[:, cols] * factors[0][:, g : g + 1]
                + swapped_ref[:, cols] * factors[1][:, g : g + 1]
            )
        lane = iotas((side_rows, STAT))[1]
        field, head = div(lane, SLOT), mod(lane, SLOT)
        tops = by_row(head, [top[:, g : g + 1] for g in range(GROUP)])
        sums = by_row(head, [total[:, g : g + 1] for g in range(GROUP)])
        high = tops.astype(BF16).astype(F32)
        middle = (tops - high).astype(BF16).astype(F32)
        low = tops - high - middle
        sum_high = sums.astype(BF16).astype(F32)
        parts.append(by_row(field, [high, middle, low, sum_high, sums - sum_high]))
        packed = jnp.concatenate(parts, axis=1).astype(BF16)
        row, col = iotas((side_rows, side_rows))
        chip, k, c = div(row, HK * CAPP), mod(div(row, CAPP), HK), mod(row, CAPP)
        out_ref[...] = dot(one_hot(k * slots + chip * CAPP + c == col), packed).astype(BF16)

    return call(
        kernel,
        pltpu.VMEM((side_rows, PIECE + STAT), BF16),
        (kept, swapped),
        [VMEM, VMEM],
        limit=4,
        out_specs=VMEM,
    )


def routes(named, logits, half, pack_ref, main_ref, tail_ref, gate_ref):
    rows = len(named[0])
    per_expert = half // EXPERTS
    row, col = iotas((EXPERTS * SLOT, HK * rows))
    expert, i, k, r = div(row, SLOT), mod(row, SLOT), div(col, rows), mod(col, rows)
    has = (by_row(r, named[0]) == expert) | (by_row(r, named[1]) == expert)
    a, b = iotas((HK * rows, HK * rows))
    earlier = (div(a, rows) == div(b, rows)) & (mod(a, rows) < mod(b, rows))
    rank = dot(one_hot(has), one_hot(earlier)).astype(jnp.int32)
    for n in range(BLOCKS):
        slot = jnp.where(i < CAPE, i, (i - CAPE) * PER + n)
        piece = jnp.where(i < CAPE, n, HK - 1)
        pack_ref[n] = one_hot(has & (rank == slot) & (k == piece))

    row, col = iotas((2 * rows, half * SLOT))
    j, r = div(row, rows), mod(row, rows)
    expert, i = div(div(col, SLOT), per_expert), mod(col, SLOT)
    mine = jnp.where(j == 0, by_row(r, named[0]), by_row(r, named[1]))
    rank = jnp.zeros(row.shape, jnp.int32)
    for q in range(rows):
        same = (mine == named[0][q]) | (mine == named[1][q])
        rank += ((r > q) & same).astype(jnp.int32)
    here = expert == mine
    main_ref[...] = one_hot(here & (i == rank))
    for n in range(BLOCKS):
        spot = jnp.full(row.shape, -1, jnp.int32)
        for m in range(SLOT - CAPE):
            spot = jnp.where(rank == m * PER + n, CAPE + m, spot)
        tail_ref[n] = one_hot(here & (i == spot))

    row, _ = iotas((rows, STAT))
    first, second = by_row(row, logits[0]), by_row(row, logits[1])
    top = jnp.maximum(first, second)
    first, second = jnp.exp(first - top), jnp.exp(second - top)
    gate_ref[0] = first / (first + second)
    gate_ref[1] = second / (first + second)


def prepare(
    queries, suffix_keys, suffix_values, lengths, prefix_of, expert_index, gate_logits,
    keys, values, hidden_in, norm_gain, devices,
):
    rows = queries.shape[0]
    half = devices // 2
    holders = half // PREFIXES
    flat = (rows * suffix_keys.shape[1], suffix_keys.shape[2])
    gain = norm_gain.reshape(1, norm_gain.shape[0])
    expert_index, gate_logits = expert_index.T, gate_logits.T

    def kernel(
        query_hbm, skey_hbm, svalue_hbm, length_hbm, prefix_hbm, expert_hbm, logit_hbm,
        key_hbm, value_hbm, hidden_hbm, gain_hbm,
        suffix_ref, stat_ref, pack_ref, main_ref, tail_ref, gate_ref, find_ref,
        key_ref, value_ref, hidden_ref, gain_ref,
        query_ref, skey_ref, svalue_ref, length_ref, prefix_ref, expert_ref, logit_ref, sems,
    ):
        copies = fetch(
            [
                (expert_hbm, expert_ref), (logit_hbm, logit_ref), (prefix_hbm, prefix_ref),
                (length_hbm, length_ref), (query_hbm, query_ref), (skey_hbm, skey_ref),
                (svalue_hbm, svalue_ref), (key_hbm, key_ref), (value_hbm, value_ref),
                (hidden_hbm, hidden_ref), (gain_hbm, gain_ref),
            ],
            sems,
        )
        start = lax.axis_index("wide") * rows
        for copy in copies[:3]:
            copy.wait()
        named = [[expert_ref[j, start + r] for r in range(rows)] for j in range(2)]
        logits = [[logit_ref[j, start + r] for r in range(rows)] for j in range(2)]
        routes(named, logits, half, pack_ref, main_ref, tail_ref, gate_ref)

        named, ranks = prefix_slots(prefix_ref, start, rows)
        firsts = [named[r] * (holders * HK * CAPP) + ranks[r] for r in range(rows)]
        row, col = iotas((HK * rows, half * HK * CAPP))
        target = by_row(mod(row, rows), firsts) + div(row, rows) * CAPP
        for h in range(holders):
            find_ref[h] = one_hot(target + h * (HK * CAPP) == col)

        for copy in copies[3:7]:
            copy.wait()
        lengths = [length_ref[r] for r in range(rows)]
        own_suffix(query_ref[...].astype(F32), skey_ref, svalue_ref, lengths, suffix_ref, stat_ref)
        for copy in copies[7:]:
            copy.wait()

    shape = jax.ShapeDtypeStruct
    return call(
        kernel,
        (
            shape((HK * rows, PIECE), F32),
            shape((HK * rows, STAT), F32),
            shape((BLOCKS, EXPERTS * SLOT, HK * rows), BF16),
            shape((2 * rows, half * SLOT), BF16),
            shape((BLOCKS, 2 * rows, half * SLOT), BF16),
            shape((2, rows, STAT), F32),
            shape((holders, HK * rows, half * HK * CAPP), BF16),
            shape(keys.shape, BF16),
            shape(values.shape, BF16),
            shape(hidden_in.shape, BF16),
            shape(gain.shape, F32),
        ),
        (
            queries, suffix_keys.reshape(flat), suffix_values.reshape(flat), lengths, prefix_of,
            expert_index, gate_logits, keys, values, hidden_in, gain,
        ),
        [HBM] * 11,
        flops=1 << 31,
        scratch=[
            pltpu.VMEM(queries.shape, BF16),
            pltpu.VMEM(flat, BF16),
            pltpu.VMEM(flat, BF16),
            pltpu.SMEM(lengths.shape, jnp.int32),
            pltpu.SMEM(prefix_of.shape, jnp.int32),
            pltpu.SMEM(expert_index.shape, jnp.int32),
            pltpu.SMEM(gate_logits.shape, F32),
            pltpu.SemaphoreType.DMA((11,)),
        ],
        limit=8,
    )


def merge(back, suffix_out, suffix_stat, hidden_in, gain, find, pack, devices):
    rows, width = hidden_in.shape
    half = devices // 2
    per_expert = half // EXPERTS

    def kernel(
        back_ref, suffix_ref, stat_ref, hidden_ref, gain_ref, find_ref, pack_ref, out_ref, sent_ref
    ):
        stat = stat_ref[...]
        outs, tops, sums = [suffix_ref[...]], [stat[:, :SLOT]], [stat[:, SLOT : 2 * SLOT]]
        for h in range(find_ref.shape[0]):
            found = dot(find_ref[h], back_ref[...])
            stat = found[:, PIECE:]
            field = [stat[:, n * SLOT : (n + 1) * SLOT] for n in range(5)]
            outs.append(found[:, :PIECE])
            tops.append(field[0] + field[1] + field[2])
            sums.append(field[3] + field[4])
        overall = tops[0]
        for top in tops[1:]:
            overall = jnp.maximum(overall, top)
        factors = [jnp.exp(top - overall) for top in tops]
        scale = 1.0 / sum(f * s for f, s in zip(factors, sums))
        factors = [f * scale for f in factors]
        merged = []
        for g in range(GROUP):
            cols = slice(g * DH, (g + 1) * DH)
            merged.append(sum(o[:, cols] * f[:, g : g + 1] for o, f in zip(outs, factors)))
        attended = jnp.concatenate(merged, axis=1).astype(BF16).astype(F32)
        for k in range(HK):
            out_ref[:, pl.ds(k * PIECE, PIECE)] = attended[k * rows : (k + 1) * rows].astype(BF16)
        stream = stack_pieces(hidden_ref[...].astype(F32)) + attended
        squares = jnp.sum(stream * stream, axis=-1, keepdims=True)
        mean = sum(squares[k * rows : (k + 1) * rows] for k in range(HK)) * (1.0 / width)
        scale = jnp.concatenate([lax.rsqrt(mean + 1e-05)] * HK, axis=0)
        gain = jnp.concatenate(
            [
                jnp.broadcast_to(gain_ref[:, k * PIECE : (k + 1) * PIECE], (rows, PIECE))
                for k in range(HK)
            ],
            axis=0,
        )
        normed = (stream * scale * gain).astype(BF16)
        for n in range(BLOCKS):
            taken = dot(pack_ref[n], normed)
            for i in range(half):
                e = i // per_expert
                sent_ref[pl.ds(i * SLOT, SLOT), pl.ds(n * PIECE, PIECE)] = taken[
                    e * SLOT : (e + 1) * SLOT
                ].astype(BF16)

    return call(
        kernel,
        (
            jax.ShapeDtypeStruct((rows, width), BF16),
            jax.ShapeDtypeStruct((half * SLOT, BLOCKS * PIECE), BF16),
        ),
        (back, suffix_out, suffix_stat, hidden_in, gain, find, pack),
        [VMEM] * 7,
        limit=8,
    )


def cuts(total, step):
    return [(p, min(step, total - p)) for p in range(0, total, step)]


def experts(near, far, gate_weight, up_weight, down_weight):
    half = near.shape[0]
    units, width = down_weight.shape
    depth = 4
    unit_cuts = cuts(units, 512)
    out_cuts = cuts(width, 512)

    def kernel(
        near_ref, far_ref, gate_hbm, up_hbm, down_hbm, mine_ref, theirs_ref,
        gate_ref, up_ref, down_ref, rows_ref, hidden_ref, sems,
    ):
        copies = []
        for p, step in unit_cuts:
            copies.append((gate_hbm, gate_ref, pl.ds(p, step)))
            copies.append((up_hbm, up_ref, pl.ds(p, step)))
        for p, step in out_cuts:
            copies.append((down_hbm, down_ref, pl.ds(p, step)))

        def copy(n):
            source, target, cols = copies[n]
            return pltpu.make_async_copy(source.at[:, cols], target.at[:, cols], sems.at[n])

        for n in range(min(depth, len(copies))):
            copy(n).start()

        def arrive(n):
            copy(n).wait()
            if n + depth < len(copies):
                copy(n + depth).start()

        row, col = iotas((half, half))
        i, i_from = mod(row, SLOT), mod(col, SLOT)
        same = div(row, SLOT) == div(col, SLOT)
        for side, ref in enumerate((near_ref, far_ref)):
            own = pl.ds(side * half, half)
            tail = jnp.zeros((half, PIECE), F32)
            for n in range(BLOCKS):
                spot = jnp.full(row.shape, -1, jnp.int32)
                for m in range(SLOT - CAPE):
                    spot = jnp.where(i == m * PER + n, CAPE + m, spot)
                tail += dot(one_hot(same & (i_from == spot)), ref[:, n * PIECE : (n + 1) * PIECE])
            rows_ref[own, : BLOCKS * PIECE] = ref[...]
            rows_ref[own, BLOCKS * PIECE :] = tail.astype(BF16)
        for n, (p, step) in enumerate(unit_cuts):
            cols = pl.ds(p, step)
            arrive(2 * n)
            gate = dot(rows_ref[...], gate_ref[:, cols])
            arrive(2 * n + 1)
            up = dot(rows_ref[...], up_ref[:, cols])
            hidden_ref[:, cols] = (gate / (1.0 + jnp.exp(-gate)) * up).astype(BF16)
        for n, (p, step) in enumerate(out_cuts):
            cols = pl.ds(p, step)
            arrive(2 * len(unit_cuts) + n)
            part = dot(hidden_ref[...], down_ref[:, cols])
            mine_ref[:, cols] = part[:half]
            theirs_ref[:, cols] = part[half:].astype(BF16)

    part = functools.partial(jax.ShapeDtypeStruct, (half, width))
    return call(
        kernel,
        (part(F32), part(BF16)),
        (near, far, gate_weight, up_weight, down_weight),
        [VMEM, VMEM, HBM, HBM, HBM],
        flops=12 * half * units * width,
        moved=6 * units * width,
        limit=42,
        scratch=[
            pltpu.VMEM(gate_weight.shape, BF16),
            pltpu.VMEM(up_weight.shape, BF16),
            pltpu.VMEM(down_weight.shape, BF16),
            pltpu.VMEM((2 * half, width), BF16),
            pltpu.VMEM((2 * half, units), BF16),
            pltpu.SemaphoreType.DMA((2 * len(unit_cuts) + len(out_cuts),)),
        ],
    )


def add_and_pack(mine, swapped):
    half, width = mine.shape

    def kernel(mine_ref, swapped_ref, out_ref):
        row, col = iotas((half, half))
        same = div(row, SLOT) == div(col, SLOT)
        i, i_from = mod(row, SLOT), mod(col, SLOT)
        keep = mod(iotas((half, PIECE))[0], SLOT) < CAPE
        last = pl.ds(BLOCKS * PIECE, PIECE)
        tail = (mine_ref[:, last] + swapped_ref[:, last].astype(F32)).astype(BF16)
        for n in range(BLOCKS):
            cols = pl.ds(n * PIECE, PIECE)
            moved = dot(one_hot(same & (i >= CAPE) & (i_from == (i - CAPE) * PER + n)), tail)
            out_ref[:, cols] = jnp.where(keep, mine_ref[:, cols] + swapped_ref[:, cols].astype(F32), moved).astype(BF16)

    return call(
        kernel,
        jax.ShapeDtypeStruct((half, BLOCKS * PIECE), BF16),
        (mine, swapped),
        [VMEM, VMEM],
    )


def mix(parts, main, tail, gates):
    rows = main.shape[0] // 2

    def kernel(part_ref, main_ref, tail_ref, gate_ref, out_ref):
        first, second = gate_ref[0][:, :1], gate_ref[1][:, :1]
        last = jnp.zeros((2 * rows, PIECE), F32)
        for n in range(BLOCKS):
            cols = pl.ds(n * PIECE, PIECE)
            found = dot(main_ref[...], part_ref[:, cols])
            out_ref[:, cols] = (found[:rows] * first + found[rows:] * second).astype(BF16)
            last += dot(tail_ref[n], part_ref[:, cols])
        cols = pl.ds(BLOCKS * PIECE, PIECE)
        out_ref[:, cols] = (last[:rows] * first + last[rows:] * second).astype(BF16)

    return call(
        kernel,
        jax.ShapeDtypeStruct((rows, HK * PIECE), BF16),
        (parts, main, tail, gates),
        [VMEM, VMEM, VMEM, VMEM],
    )


def exchange(x, groups):
    return lax.all_to_all(x, "wide", 0, 0, tiled=True, axis_index_groups=groups)


def local(
    queries,
    hidden_in,
    prefix_keys,
    prefix_values,
    suffix_keys,
    suffix_values,
    suffix_length,
    prefix_of,
    expert_index,
    gate_logits,
    norm_gain,
    gate_weight,
    up_weight,
    down_weight,
):
    devices = lax.axis_size("wide")
    rows = queries.shape[0]
    half = devices // 2
    siblings = [(i, i ^ 1) for i in range(devices)]
    alike = [[2 * i + c for i in range(half)] for c in range(2)]
    prefix_of = prefix_of[:, 0]

    outgoing = send_queries(queries, prefix_of, devices)
    outgoing, suffix_length = lax.optimization_barrier((outgoing, suffix_length))
    near = exchange(outgoing, alike)
    suffix_out, suffix_stat, pack, main, tail, gates, find, keys, values, hidden, gain = prepare(
        queries, suffix_keys, suffix_values, suffix_length, prefix_of, expert_index, gate_logits,
        prefix_keys, prefix_values, hidden_in, norm_gain, devices,
    )
    near, keys = lax.optimization_barrier((near, keys))
    far = lax.ppermute(near, "wide", siblings)
    kept, given = prefix_block(near, far, keys, values)
    swapped = lax.ppermute(given, "wide", siblings)
    back = exchange(join_blocks(kept, swapped), alike)
    attended, sent = merge(back, suffix_out, suffix_stat, hidden, gain, find, pack, devices)
    near = exchange(sent, alike)
    far = lax.ppermute(near, "wide", siblings)
    mine, theirs = experts(near, far, gate_weight, up_weight, down_weight)
    swapped = lax.ppermute(theirs, "wide", siblings)
    parts = exchange(add_and_pack(mine, swapped), alike)
    return attended, mix(parts, main, tail, gates)


def solution(mesh):
    placed = (
        P(("groups", "wide"), None),
        P(("groups", "wide"), None),
        P(("groups", "wide"), None),
        P(("groups", "wide"), None),
        P(("groups", "wide"), None, None),
        P(("groups", "wide"), None, None),
        P(("groups", "wide")),
        P("groups", None),
        P("groups", None),
        P("groups", None),
        P(),
        P(None, "wide"),
        P(None, "wide"),
        P("wide", None),
    )
    return jax.shard_map(
        local,
        mesh=mesh,
        in_specs=placed,
        out_specs=(P(("groups", "wide"), None), P(("groups", "wide"), None)),
        check_vma=False,
    )
```

```python
import functools
import math

import jax
import jax.numpy as jnp
from jax import lax
from jax.experimental import pallas as pl
from jax.experimental.pallas import tpu as pltpu
from jax.sharding import PartitionSpec as P

HQ = 24
HK = 4
DH = 128
EXPERTS = 4
PREFIXES = 8
CAPP = 2
CAPE = 6

GROUP = HQ // HK
PIECE = GROUP * DH
STAT = 128
SLOT = 8
BLOCKS = CAPE * HK // SLOT
PER = CAPE // (SLOT - CAPE)

masked_score = -1e30
F32 = jnp.float32
BF16 = jnp.bfloat16
VMEM = pl.BlockSpec(memory_space=pltpu.VMEM)
SMEM = pl.BlockSpec(memory_space=pltpu.SMEM)
HBM = pl.BlockSpec(memory_space=pltpu.HBM)


def iotas(shape):
    return lax.broadcasted_iota(jnp.int32, shape, 0), lax.broadcasted_iota(jnp.int32, shape, 1)


def div(x, m):
    return jnp.right_shift(x, m.bit_length() - 1)


def mod(x, m):
    return jnp.bitwise_and(x, m - 1)


def one_hot(picked):
    return picked.astype(F32).astype(BF16)


def dot(a, b):
    return jnp.dot(a, b, preferred_element_type=F32)


def dot_t(a, b):
    return lax.dot_general(a, b, (((1,), (1,)), ((), ())), preferred_element_type=F32)


def by_row(index, values):
    out = jnp.zeros(index.shape, jnp.asarray(values[0]).dtype)
    for i, value in enumerate(values):
        out = jnp.where(index == i, value, out)
    return out


def prefix_slots(prefix_ref, start, rows):
    named = [prefix_ref[start + r] for r in range(rows)]
    ranks = []
    for r in range(rows):
        rank = jnp.int32(0)
        for q in range(r):
            rank += (named[q] == named[r]).astype(jnp.int32)
        ranks.append(rank)
    return named, ranks


def stack_pieces(x):
    return jnp.concatenate([x[:, k * PIECE : (k + 1) * PIECE] for k in range(HK)], axis=0)


def call(kernel, outs, ins, specs, flops=0, limit=24, scratch=(), moved=0, out_specs=None):
    ins = [pltpu.with_memory_space_constraint(x, pltpu.HBM) if s is HBM else x for x, s in zip(ins, specs)]
    return pl.pallas_call(
        kernel,
        out_shape=outs,
        in_specs=specs,
        out_specs=out_specs or jax.tree.map(lambda _: VMEM, outs),
        scratch_shapes=scratch,
        compiler_params=pltpu.CompilerParams(vmem_limit_bytes=limit * 1024 * 1024),
        cost_estimate=pl.CostEstimate(
            flops=flops, bytes_accessed=moved or 1 << 20, transcendentals=0
        ),
    )(*ins)


def fetch(pairs, sems):
    copies = [pltpu.make_async_copy(s, t, sems.at[n]) for n, (s, t) in enumerate(pairs)]
    for copy in copies:
        copy.start()
    return copies


def send_queries(queries, prefix_of, devices):
    rows = queries.shape[0]
    chips = devices // 2
    holders = devices // 2 // PREFIXES

    def kernel(query_hbm, prefix_hbm, out_ref, query_ref, prefix_ref, sems):
        copies = fetch([(prefix_hbm, prefix_ref), (query_hbm, query_ref)], sems)
        row, col = iotas((chips * HK * CAPP, HK * rows))
        chip, k, c = div(row, HK * CAPP), mod(div(row, CAPP), HK), mod(row, CAPP)
        r = mod(col, rows)
        copies[0].wait()
        start = lax.axis_index("wide") * rows
        named, ranks = prefix_slots(prefix_ref, start, rows)
        picked = (
            (k == div(col, rows)) & (div(chip, holders) == by_row(r, named)) & (c == by_row(r, ranks))
        )
        copies[1].wait()
        pieces = stack_pieces(query_ref[...].astype(F32)).astype(BF16)
        out_ref[...] = dot(one_hot(picked), pieces).astype(BF16)

    return call(
        kernel,
        pltpu.VMEM((chips * HK * CAPP, PIECE), BF16),
        (queries, prefix_of),
        [HBM, HBM],
        scratch=[
            pltpu.VMEM(queries.shape, BF16),
            pltpu.SMEM(prefix_of.shape, jnp.int32),
            pltpu.SemaphoreType.DMA((2,)),
        ],
        limit=4,
        out_specs=VMEM,
    )


def softmax_block(query, keys, values, mask):
    scores = dot_t(query, keys) * (1.0 / math.sqrt(DH))
    if mask is not None:
        scores = jnp.where(mask, scores, masked_score)
    top = jnp.max(scores, axis=-1, keepdims=True)
    weights = jnp.exp(scores - top).astype(BF16)
    total = jnp.sum(weights.astype(F32), axis=-1, keepdims=True)
    return dot(weights, values), top, total


def heads_of(x):
    return jnp.concatenate([x[:, g * DH : (g + 1) * DH] for g in range(GROUP)], axis=0)


def own_suffix(query, key_ref, value_ref, live, out_ref, stat_ref):
    rows = query.shape[0]
    mask = jnp.concatenate([live] * GROUP, axis=0) > 0.5
    lane = iotas((rows, STAT))[1]
    for k in range(HK):
        cols = pl.ds(k * DH, DH)
        own = pl.ds(k * rows, rows)
        out, top, total = softmax_block(
            heads_of(query[:, k * PIECE : (k + 1) * PIECE]).astype(BF16),
            key_ref[:, cols],
            value_ref[:, cols],
            mask,
        )
        stat = jnp.zeros((rows, STAT), F32)
        for g in range(GROUP):
            part = slice(g * rows, (g + 1) * rows)
            out_ref[own, pl.ds(g * DH, DH)] = out[part]
            stat = jnp.where(lane == g, top[part], stat)
            stat = jnp.where(lane == SLOT + g, total[part], stat)
        stat_ref[own, :] = stat


def stats_of(field, head, tops, sums):
    return by_row(field, [by_row(head, tops), by_row(head, sums)])


def prefix_block(near, far, keys, values):
    side_rows = near.shape[0]
    total_rows = 2 * side_rows
    slots = total_rows // HK
    half = slots // 2

    def kernel(near_ref, far_ref, key_ref, value_ref, kept_ref, given_ref):
        row, col = iotas((total_rows, side_rows))
        k, slot = div(row, slots), mod(row, slots)
        side, slot = div(slot, half), mod(slot, half)
        source = div(slot, CAPP) * (HK * CAPP) + k * CAPP + mod(slot, CAPP)
        query = dot(one_hot((side == 0) & (source == col)), near_ref[...]) + dot(
            one_hot((side == 1) & (source == col)), far_ref[...]
        )
        lane = iotas((slots, STAT))[1]
        field, head = div(lane, SLOT), mod(lane, SLOT)
        for k in range(HK):
            cols = pl.ds(k * DH, DH)
            out, top, total = softmax_block(
                heads_of(query[k * slots : (k + 1) * slots]).astype(BF16),
                key_ref[:, cols],
                value_ref[:, cols],
                None,
            )
            tops = [top[g * slots : (g + 1) * slots] for g in range(GROUP)]
            sums = [total[g * slots : (g + 1) * slots] for g in range(GROUP)]
            stat = stats_of(field, head, tops, sums)
            own = pl.ds(k * half, half)
            for side, ref in enumerate((kept_ref, given_ref)):
                for g in range(GROUP):
                    first = g * slots + side * half
                    ref[own, pl.ds(g * DH, DH)] = out[first : first + half]
                ref[own, pl.ds(PIECE, STAT)] = stat[side * half : (side + 1) * half]

    part = jax.ShapeDtypeStruct((side_rows, PIECE + STAT), F32)
    return call(
        kernel,
        (part, part),
        (near, far, keys, values),
        [VMEM] * 4,
        limit=8,
    )


def join_blocks(kept, swapped):
    side_rows = kept.shape[0]
    slots = side_rows // HK

    def kernel(kept_ref, swapped_ref, out_ref):
        stat = [ref[:, PIECE:] for ref in (kept_ref, swapped_ref)]
        tops, sums = [s[:, :SLOT] for s in stat], [s[:, SLOT : 2 * SLOT] for s in stat]
        top = jnp.maximum(*tops)
        factors = [jnp.exp(t - top) for t in tops]
        total = factors[0] * sums[0] + factors[1] * sums[1]
        parts = []
        for g in range(GROUP):
            cols = pl.ds(g * DH, DH)
            parts.append(
                kept_ref[:, cols] * factors[0][:, g : g + 1]
                + swapped_ref[:, cols] * factors[1][:, g : g + 1]
            )
        lane = iotas((side_rows, STAT))[1]
        field, head = div(lane, SLOT), mod(lane, SLOT)
        tops = by_row(head, [top[:, g : g + 1] for g in range(GROUP)])
        sums = by_row(head, [total[:, g : g + 1] for g in range(GROUP)])
        high = tops.astype(BF16).astype(F32)
        middle = (tops - high).astype(BF16).astype(F32)
        low = tops - high - middle
        sum_high = sums.astype(BF16).astype(F32)
        parts.append(by_row(field, [high, middle, low, sum_high, sums - sum_high]))
        packed = jnp.concatenate(parts, axis=1).astype(BF16)
        row, col = iotas((side_rows, side_rows))
        chip, k, c = div(row, HK * CAPP), mod(div(row, CAPP), HK), mod(row, CAPP)
        out_ref[...] = dot(one_hot(k * slots + chip * CAPP + c == col), packed).astype(BF16)

    return call(
        kernel,
        pltpu.VMEM((side_rows, PIECE + STAT), BF16),
        (kept, swapped),
        [VMEM, VMEM],
        limit=4,
        out_specs=VMEM,
    )


def routes_out(named, pack_ref):
    rows = len(named[0])
    row, col = iotas((EXPERTS * SLOT, HK * rows))
    expert, i, k, r = div(row, SLOT), mod(row, SLOT), div(col, rows), mod(col, rows)
    has = (by_row(r, named[0]) == expert) | (by_row(r, named[1]) == expert)
    a, b = iotas((HK * rows, HK * rows))
    earlier = (div(a, rows) == div(b, rows)) & (mod(a, rows) < mod(b, rows))
    rank = dot(one_hot(has), one_hot(earlier)).astype(jnp.int32)
    for n in range(BLOCKS):
        slot = jnp.where(i < CAPE, i, (i - CAPE) * PER + n)
        piece = jnp.where(i < CAPE, n, HK - 1)
        pack_ref[n] = one_hot(has & (rank == slot) & (k == piece))


def routes_back(named, logits, half, main_ref, tail_ref, gate_ref):
    rows = len(named[0])
    per_expert = half // EXPERTS
    row, col = iotas((2 * rows, half * SLOT))
    j, r = div(row, rows), mod(row, rows)
    expert, i = div(div(col, SLOT), per_expert), mod(col, SLOT)
    mine = jnp.where(j == 0, by_row(r, named[0]), by_row(r, named[1]))
    rank = jnp.zeros(row.shape, jnp.int32)
    for q in range(rows):
        same = (mine == named[0][q]) | (mine == named[1][q])
        rank += ((r > q) & same).astype(jnp.int32)
    here = expert == mine
    main_ref[...] = one_hot(here & (i == rank))
    for n in range(BLOCKS):
        spot = jnp.full(row.shape, -1, jnp.int32)
        for m in range(SLOT - CAPE):
            spot = jnp.where(rank == m * PER + n, CAPE + m, spot)
        tail_ref[n] = one_hot(here & (i == spot))

    row, _ = iotas((rows, STAT))
    first, second = by_row(row, logits[0]), by_row(row, logits[1])
    top = jnp.maximum(first, second)
    first, second = jnp.exp(first - top), jnp.exp(second - top)
    gate_ref[0] = first / (first + second)
    gate_ref[1] = second / (first + second)


def own_experts(expert_ref, start, rows):
    return [[expert_ref[j, start + r] for r in range(rows)] for j in range(2)]


def stage(prefix_of, expert_index, lengths, arrays, after, devices, rows, span):
    half = devices // 2
    holders = half // PREFIXES
    expert_index = expert_index.T
    count = len(arrays)

    def kernel(*refs):
        _, prefix_hbm, expert_hbm, length_hbm = refs[:4]
        sources, outs = refs[4 : 4 + count], refs[4 + count : 4 + 2 * count]
        find_ref, pack_ref, live_ref, prefix_ref, expert_ref, length_ref, sems = refs[4 + 2 * count :]
        copies = fetch(
            [
                (prefix_hbm, prefix_ref), (expert_hbm, expert_ref), (length_hbm, length_ref),
                *zip(sources, outs),
            ],
            sems,
        )
        start = lax.axis_index("wide") * rows
        for copy in copies[:3]:
            copy.wait()
        row, col = iotas((rows, rows * span))
        owner = div(col, span)
        length = by_row(owner, [length_ref[r] for r in range(rows)])
        live_ref[...] = ((owner == row) & (mod(col, span) < length)).astype(F32)
        named, ranks = prefix_slots(prefix_ref, start, rows)
        firsts = [named[r] * (holders * HK * CAPP) + ranks[r] for r in range(rows)]
        row, col = iotas((HK * rows, half * HK * CAPP))
        target = by_row(mod(row, rows), firsts) + div(row, rows) * CAPP
        for h in range(holders):
            find_ref[h] = one_hot(target + h * (HK * CAPP) == col)
        routes_out(own_experts(expert_ref, start, rows), pack_ref)
        for copy in copies[3:]:
            copy.wait()

    return call(
        kernel,
        (
            *[pltpu.VMEM(x.shape, x.dtype) for x in arrays],
            pltpu.VMEM((holders, HK * rows, half * HK * CAPP), BF16),
            pltpu.VMEM((BLOCKS, EXPERTS * SLOT, HK * rows), BF16),
            pltpu.VMEM((rows, rows * span), F32),
        ),
        (after, prefix_of, expert_index, lengths, *arrays),
        [VMEM] + [HBM] * (3 + count),
        flops=1 << 30,
        scratch=[
            pltpu.SMEM(prefix_of.shape, jnp.int32),
            pltpu.SMEM(expert_index.shape, jnp.int32),
            pltpu.SMEM(lengths.shape, jnp.int32),
            pltpu.SemaphoreType.DMA((3 + count,)),
        ],
        out_specs=(VMEM,) * (3 + count),
        limit=4,
    )


def suffix_block(queries, keys, values, live, after):
    rows = queries.shape[0]

    def kernel(_, query_ref, key_ref, value_ref, live_ref, out_ref, stat_ref):
        own_suffix(
            query_ref[...].astype(F32), key_ref, value_ref, live_ref[...], out_ref, stat_ref
        )

    return call(
        kernel,
        (pltpu.VMEM((HK * rows, PIECE), F32), pltpu.VMEM((HK * rows, STAT), F32)),
        (after, queries, keys, values, live),
        [VMEM] * 5,
        flops=1 << 30,
        out_specs=(VMEM, VMEM),
        limit=4,
    )


def finish(attended, expert_index, gate_logits, after, devices):
    rows = attended.shape[0]
    half = devices // 2
    expert_index, gate_logits = expert_index.T, gate_logits.T

    def kernel(
        _, attended_ref, expert_hbm, logit_hbm,
        out_hbm, main_ref, tail_ref, gate_ref, expert_ref, logit_ref, sems,
    ):
        copies = fetch(
            [(expert_hbm, expert_ref), (logit_hbm, logit_ref), (attended_ref, out_hbm)], sems
        )
        start = lax.axis_index("wide") * rows
        for copy in copies[:2]:
            copy.wait()
        named = own_experts(expert_ref, start, rows)
        logits = own_experts(logit_ref, start, rows)
        routes_back(named, logits, half, main_ref, tail_ref, gate_ref)
        copies[2].wait()

    return call(
        kernel,
        (
            pltpu.HBM(attended.shape, attended.dtype),
            pltpu.VMEM((2 * rows, half * SLOT), BF16),
            pltpu.VMEM((BLOCKS, 2 * rows, half * SLOT), BF16),
            pltpu.VMEM((2, rows, STAT), F32),
        ),
        (after, attended, expert_index, gate_logits),
        [VMEM, VMEM, HBM, HBM],
        flops=1 << 30,
        scratch=[
            pltpu.SMEM(expert_index.shape, jnp.int32),
            pltpu.SMEM(gate_logits.shape, F32),
            pltpu.SemaphoreType.DMA((3,)),
        ],
        out_specs=(HBM, VMEM, VMEM, VMEM),
        limit=4,
    )


def merge(back, suffix_out, suffix_stat, hidden_in, gain, find, pack, devices):
    rows, width = hidden_in.shape
    half = devices // 2
    per_expert = half // EXPERTS

    def kernel(
        back_ref, suffix_ref, stat_ref, hidden_ref, gain_ref, find_ref, pack_ref, out_ref, sent_ref
    ):
        stat = stat_ref[...]
        outs, tops, sums = [suffix_ref[...]], [stat[:, :SLOT]], [stat[:, SLOT : 2 * SLOT]]
        for h in range(find_ref.shape[0]):
            found = dot(find_ref[h], back_ref[...])
            stat = found[:, PIECE:]
            field = [stat[:, n * SLOT : (n + 1) * SLOT] for n in range(5)]
            outs.append(found[:, :PIECE])
            tops.append(field[0] + field[1] + field[2])
            sums.append(field[3] + field[4])
        overall = tops[0]
        for top in tops[1:]:
            overall = jnp.maximum(overall, top)
        factors = [jnp.exp(top - overall) for top in tops]
        scale = 1.0 / sum(f * s for f, s in zip(factors, sums))
        factors = [f * scale for f in factors]
        merged = []
        for g in range(GROUP):
            cols = slice(g * DH, (g + 1) * DH)
            merged.append(sum(o[:, cols] * f[:, g : g + 1] for o, f in zip(outs, factors)))
        attended = jnp.concatenate(merged, axis=1).astype(BF16).astype(F32)
        for k in range(HK):
            out_ref[:, pl.ds(k * PIECE, PIECE)] = attended[k * rows : (k + 1) * rows].astype(BF16)
        stream = stack_pieces(hidden_ref[...].astype(F32)) + attended
        squares = jnp.sum(stream * stream, axis=-1, keepdims=True)
        mean = sum(squares[k * rows : (k + 1) * rows] for k in range(HK)) * (1.0 / width)
        scale = jnp.concatenate([lax.rsqrt(mean + 1e-05)] * HK, axis=0)
        gain = jnp.concatenate(
            [
                jnp.broadcast_to(gain_ref[:, k * PIECE : (k + 1) * PIECE], (rows, PIECE))
                for k in range(HK)
            ],
            axis=0,
        )
        normed = (stream * scale * gain).astype(BF16)
        for n in range(BLOCKS):
            taken = dot(pack_ref[n], normed)
            for i in range(half):
                e = i // per_expert
                sent_ref[pl.ds(i * SLOT, SLOT), pl.ds(n * PIECE, PIECE)] = taken[
                    e * SLOT : (e + 1) * SLOT
                ].astype(BF16)

    return call(
        kernel,
        (
            pltpu.VMEM((rows, width), BF16),
            pltpu.VMEM((half * SLOT, BLOCKS * PIECE), BF16),
        ),
        (back, suffix_out, suffix_stat, hidden_in, gain, find, pack),
        [VMEM] * 7,
        limit=8,
        out_specs=(VMEM, VMEM),
    )


def cuts(total, step):
    return [(p, min(step, total - p)) for p in range(0, total, step)]


def experts(near, far, gate_weight, up_weight, down_weight):
    half = near.shape[0]
    units, width = down_weight.shape
    depth = 4
    unit_cuts = cuts(units, 512)
    out_cuts = cuts(width, 512)

    def kernel(
        near_ref, far_ref, gate_hbm, up_hbm, down_hbm, mine_ref, theirs_ref,
        gate_ref, up_ref, down_ref, rows_ref, hidden_ref, sems,
    ):
        copies = []
        for p, step in unit_cuts:
            copies.append((gate_hbm, gate_ref, pl.ds(p, step)))
            copies.append((up_hbm, up_ref, pl.ds(p, step)))
        for p, step in out_cuts:
            copies.append((down_hbm, down_ref, pl.ds(p, step)))

        def copy(n):
            source, target, cols = copies[n]
            return pltpu.make_async_copy(source.at[:, cols], target.at[:, cols], sems.at[n])

        for n in range(min(depth, len(copies))):
            copy(n).start()

        def arrive(n):
            copy(n).wait()
            if n + depth < len(copies):
                copy(n + depth).start()

        row, col = iotas((half, half))
        i, i_from = mod(row, SLOT), mod(col, SLOT)
        same = div(row, SLOT) == div(col, SLOT)
        for side, ref in enumerate((near_ref, far_ref)):
            own = pl.ds(side * half, half)
            tail = jnp.zeros((half, PIECE), F32)
            for n in range(BLOCKS):
                spot = jnp.full(row.shape, -1, jnp.int32)
                for m in range(SLOT - CAPE):
                    spot = jnp.where(i == m * PER + n, CAPE + m, spot)
                tail += dot(one_hot(same & (i_from == spot)), ref[:, n * PIECE : (n + 1) * PIECE])
            rows_ref[own, : BLOCKS * PIECE] = ref[...]
            rows_ref[own, BLOCKS * PIECE :] = tail.astype(BF16)
        for n, (p, step) in enumerate(unit_cuts):
            cols = pl.ds(p, step)
            arrive(2 * n)
            gate = dot(rows_ref[...], gate_ref[:, cols])
            arrive(2 * n + 1)
            up = dot(rows_ref[...], up_ref[:, cols])
            hidden_ref[:, cols] = (gate / (1.0 + jnp.exp(-gate)) * up).astype(BF16)
        for n, (p, step) in enumerate(out_cuts):
            cols = pl.ds(p, step)
            arrive(2 * len(unit_cuts) + n)
            part = dot(hidden_ref[...], down_ref[:, cols])
            mine_ref[:, cols] = part[:half]
            theirs_ref[:, cols] = part[half:].astype(BF16)

    part = functools.partial(jax.ShapeDtypeStruct, (half, width))
    return call(
        kernel,
        (part(F32), part(BF16)),
        (near, far, gate_weight, up_weight, down_weight),
        [VMEM, VMEM, HBM, HBM, HBM],
        flops=12 * half * units * width,
        moved=6 * units * width,
        limit=42,
        scratch=[
            pltpu.VMEM(gate_weight.shape, BF16),
            pltpu.VMEM(up_weight.shape, BF16),
            pltpu.VMEM(down_weight.shape, BF16),
            pltpu.VMEM((2 * half, width), BF16),
            pltpu.VMEM((2 * half, units), BF16),
            pltpu.SemaphoreType.DMA((2 * len(unit_cuts) + len(out_cuts),)),
        ],
    )


def add_and_pack(mine, swapped):
    half, width = mine.shape

    def kernel(mine_ref, swapped_ref, out_ref):
        row, col = iotas((half, half))
        same = div(row, SLOT) == div(col, SLOT)
        i, i_from = mod(row, SLOT), mod(col, SLOT)
        keep = mod(iotas((half, PIECE))[0], SLOT) < CAPE
        last = pl.ds(BLOCKS * PIECE, PIECE)
        tail = (mine_ref[:, last] + swapped_ref[:, last].astype(F32)).astype(BF16)
        for n in range(BLOCKS):
            cols = pl.ds(n * PIECE, PIECE)
            moved = dot(one_hot(same & (i >= CAPE) & (i_from == (i - CAPE) * PER + n)), tail)
            out_ref[:, cols] = jnp.where(keep, mine_ref[:, cols] + swapped_ref[:, cols].astype(F32), moved).astype(BF16)

    return call(
        kernel,
        jax.ShapeDtypeStruct((half, BLOCKS * PIECE), BF16),
        (mine, swapped),
        [VMEM, VMEM],
    )


def mix(parts, main, tail, gates):
    rows = main.shape[0] // 2

    def kernel(part_ref, main_ref, tail_ref, gate_ref, out_ref):
        first, second = gate_ref[0][:, :1], gate_ref[1][:, :1]
        last = jnp.zeros((2 * rows, PIECE), F32)
        for n in range(BLOCKS):
            cols = pl.ds(n * PIECE, PIECE)
            found = dot(main_ref[...], part_ref[:, cols])
            out_ref[:, cols] = (found[:rows] * first + found[rows:] * second).astype(BF16)
            last += dot(tail_ref[n], part_ref[:, cols])
        cols = pl.ds(BLOCKS * PIECE, PIECE)
        out_ref[:, cols] = (last[:rows] * first + last[rows:] * second).astype(BF16)

    return call(
        kernel,
        jax.ShapeDtypeStruct((rows, HK * PIECE), BF16),
        (parts, main, tail, gates),
        [VMEM, VMEM, VMEM, VMEM],
    )


def exchange(x, groups):
    return lax.all_to_all(x, "wide", 0, 0, tiled=True, axis_index_groups=groups)


def local(
    queries,
    hidden_in,
    prefix_keys,
    prefix_values,
    suffix_keys,
    suffix_values,
    suffix_length,
    prefix_of,
    expert_index,
    gate_logits,
    norm_gain,
    gate_weight,
    up_weight,
    down_weight,
):
    devices = lax.axis_size("wide")
    rows = queries.shape[0]
    half = devices // 2
    siblings = [(i, i ^ 1) for i in range(devices)]
    alike = [[2 * i + c for i in range(half)] for c in range(2)]
    prefix_of = prefix_of[:, 0]

    outgoing = send_queries(queries, prefix_of, devices)
    near = exchange(outgoing, alike)
    far = lax.ppermute(near, "wide", siblings)
    flat = (-1, suffix_keys.shape[2])
    keys, values, suffix_keys, suffix_values, own, hidden, gain, find, pack, live = stage(
        prefix_of,
        expert_index,
        suffix_length,
        (
            prefix_keys, prefix_values, suffix_keys.reshape(flat), suffix_values.reshape(flat),
            queries, hidden_in, norm_gain.reshape(1, -1),
        ),
        near,
        devices,
        rows,
        suffix_keys.shape[1],
    )
    kept, given = prefix_block(near, far, keys, values)
    swapped = lax.ppermute(given, "wide", siblings)
    suffix_out, suffix_stat = suffix_block(own, suffix_keys, suffix_values, live, kept)
    swapped, suffix_stat = lax.optimization_barrier((swapped, suffix_stat))
    back = exchange(join_blocks(kept, swapped), alike)
    attended, sent = merge(back, suffix_out, suffix_stat, hidden, gain, find, pack, devices)
    near = exchange(sent, alike)
    far = lax.ppermute(near, "wide", siblings)
    attended, main, tail, gates = finish(attended, expert_index, gate_logits, near, devices)
    far, gates = lax.optimization_barrier((far, gates))
    mine, theirs = experts(near, far, gate_weight, up_weight, down_weight)
    swapped = lax.ppermute(theirs, "wide", siblings)
    parts = exchange(add_and_pack(mine, swapped), alike)
    return attended, mix(parts, main, tail, gates)


def solution(mesh):
    placed = (
        P(("groups", "wide"), None),
        P(("groups", "wide"), None),
        P(("groups", "wide"), None),
        P(("groups", "wide"), None),
        P(("groups", "wide"), None, None),
        P(("groups", "wide"), None, None),
        P(("groups", "wide")),
        P("groups", None),
        P("groups", None),
        P("groups", None),
        P(),
        P(None, "wide"),
        P(None, "wide"),
        P("wide", None),
    )
    return jax.shard_map(
        local,
        mesh=mesh,
        in_specs=placed,
        out_specs=(P(("groups", "wide"), None), P(("groups", "wide"), None)),
        check_vma=False,
    )
```

```python
import functools
import math

import jax
import jax.numpy as jnp
from jax import lax
from jax.experimental import pallas as pl
from jax.experimental.pallas import tpu as pltpu
from jax.sharding import PartitionSpec as P

HQ = 24
HK = 4
DH = 128
EXPERTS = 4
PREFIXES = 8
CAPP = 2
CAPE = 6

GROUP = HQ // HK
PIECE = GROUP * DH
STAT = 128
SLOT = 8
BLOCKS = CAPE * HK // SLOT
PER = CAPE // (SLOT - CAPE)

masked_score = -1e30
F32 = jnp.float32
BF16 = jnp.bfloat16
VMEM = pl.BlockSpec(memory_space=pltpu.VMEM)
SMEM = pl.BlockSpec(memory_space=pltpu.SMEM)
HBM = pl.BlockSpec(memory_space=pltpu.HBM)


def iotas(shape):
    return lax.broadcasted_iota(jnp.int32, shape, 0), lax.broadcasted_iota(jnp.int32, shape, 1)


def div(x, m):
    return jnp.right_shift(x, m.bit_length() - 1)


def mod(x, m):
    return jnp.bitwise_and(x, m - 1)


def one_hot(picked):
    return picked.astype(F32).astype(BF16)


def dot(a, b):
    return jnp.dot(a, b, preferred_element_type=F32)


def dot_t(a, b):
    return lax.dot_general(a, b, (((1,), (1,)), ((), ())), preferred_element_type=F32)


def by_row(index, values):
    out = jnp.zeros(index.shape, jnp.asarray(values[0]).dtype)
    for i, value in enumerate(values):
        out = jnp.where(index == i, value, out)
    return out


def prefix_slots(prefix_ref, start, rows):
    named = [prefix_ref[start + r] for r in range(rows)]
    ranks = []
    for r in range(rows):
        rank = jnp.int32(0)
        for q in range(r):
            rank += (named[q] == named[r]).astype(jnp.int32)
        ranks.append(rank)
    return named, ranks


def stack_pieces(x):
    return jnp.concatenate([x[:, k * PIECE : (k + 1) * PIECE] for k in range(HK)], axis=0)


def call(kernel, outs, ins, specs, flops=0, limit=24, scratch=(), moved=0, out_specs=None):
    ins = [pltpu.with_memory_space_constraint(x, pltpu.HBM) if s is HBM else x for x, s in zip(ins, specs)]
    return pl.pallas_call(
        kernel,
        out_shape=outs,
        in_specs=specs,
        out_specs=out_specs or jax.tree.map(lambda _: VMEM, outs),
        scratch_shapes=scratch,
        compiler_params=pltpu.CompilerParams(vmem_limit_bytes=limit * 1024 * 1024),
        cost_estimate=pl.CostEstimate(
            flops=flops, bytes_accessed=moved or 1 << 20, transcendentals=0
        ),
    )(*ins)


def fetch(pairs, sems):
    copies = [pltpu.make_async_copy(s, t, sems.at[n]) for n, (s, t) in enumerate(pairs)]
    for copy in copies:
        copy.start()
    return copies


def send_queries(queries, prefix_of, devices):
    rows = queries.shape[0]
    chips = devices // 2
    holders = devices // 2 // PREFIXES

    def kernel(query_hbm, prefix_hbm, out_ref, query_ref, prefix_ref, sems):
        copies = fetch([(prefix_hbm, prefix_ref), (query_hbm, query_ref)], sems)
        row, col = iotas((chips * HK * CAPP, HK * rows))
        chip, k, c = div(row, HK * CAPP), mod(div(row, CAPP), HK), mod(row, CAPP)
        r = mod(col, rows)
        copies[0].wait()
        start = lax.axis_index("wide") * rows
        named, ranks = prefix_slots(prefix_ref, start, rows)
        picked = (
            (k == div(col, rows)) & (div(chip, holders) == by_row(r, named)) & (c == by_row(r, ranks))
        )
        copies[1].wait()
        pieces = stack_pieces(query_ref[...].astype(F32)).astype(BF16)
        out_ref[...] = dot(one_hot(picked), pieces).astype(BF16)

    return call(
        kernel,
        pltpu.VMEM((chips * HK * CAPP, PIECE), BF16),
        (queries, prefix_of),
        [HBM, HBM],
        scratch=[
            pltpu.VMEM(queries.shape, BF16),
            pltpu.SMEM(prefix_of.shape, jnp.int32),
            pltpu.SemaphoreType.DMA((2,)),
        ],
        limit=4,
        out_specs=VMEM,
    )


def softmax_block(query, keys, values, mask):
    scores = dot_t(query, keys) * (1.0 / math.sqrt(DH))
    if mask is not None:
        scores = jnp.where(mask, scores, masked_score)
    top = jnp.max(scores, axis=-1, keepdims=True)
    weights = jnp.exp(scores - top).astype(BF16)
    total = jnp.sum(weights.astype(F32), axis=-1, keepdims=True)
    return dot(weights, values), top, total


def heads_of(x):
    return jnp.concatenate([x[:, g * DH : (g + 1) * DH] for g in range(GROUP)], axis=0)


def own_suffix(query, key_ref, value_ref, live, out_ref, stat_ref):
    rows = query.shape[0]
    mask = jnp.concatenate([live] * GROUP, axis=0) > 0.5
    lane = iotas((rows, STAT))[1]
    for k in range(HK):
        cols = pl.ds(k * DH, DH)
        own = pl.ds(k * rows, rows)
        out, top, total = softmax_block(
            heads_of(query[:, k * PIECE : (k + 1) * PIECE]).astype(BF16),
            key_ref[:, cols],
            value_ref[:, cols],
            mask,
        )
        stat = jnp.zeros((rows, STAT), F32)
        for g in range(GROUP):
            part = slice(g * rows, (g + 1) * rows)
            out_ref[own, pl.ds(g * DH, DH)] = out[part]
            stat = jnp.where(lane == g, top[part], stat)
            stat = jnp.where(lane == SLOT + g, total[part], stat)
        stat_ref[own, :] = stat


def stats_of(field, head, tops, sums):
    return by_row(field, [by_row(head, tops), by_row(head, sums)])


def prefix_block(near, far, keys, values):
    side_rows = near.shape[0]
    total_rows = 2 * side_rows
    slots = total_rows // HK
    half = slots // 2

    def kernel(near_ref, far_ref, key_ref, value_ref, kept_ref, given_ref):
        row, col = iotas((total_rows, side_rows))
        k, slot = div(row, slots), mod(row, slots)
        side, slot = div(slot, half), mod(slot, half)
        source = div(slot, CAPP) * (HK * CAPP) + k * CAPP + mod(slot, CAPP)
        query = dot(one_hot((side == 0) & (source == col)), near_ref[...]) + dot(
            one_hot((side == 1) & (source == col)), far_ref[...]
        )
        lane = iotas((slots, STAT))[1]
        field, head = div(lane, SLOT), mod(lane, SLOT)
        for k in range(HK):
            cols = pl.ds(k * DH, DH)
            out, top, total = softmax_block(
                heads_of(query[k * slots : (k + 1) * slots]).astype(BF16),
                key_ref[:, cols],
                value_ref[:, cols],
                None,
            )
            tops = [top[g * slots : (g + 1) * slots] for g in range(GROUP)]
            sums = [total[g * slots : (g + 1) * slots] for g in range(GROUP)]
            stat = stats_of(field, head, tops, sums)
            own = pl.ds(k * half, half)
            for side, ref in enumerate((kept_ref, given_ref)):
                for g in range(GROUP):
                    first = g * slots + side * half
                    ref[own, pl.ds(g * DH, DH)] = out[first : first + half]
                ref[own, pl.ds(PIECE, STAT)] = stat[side * half : (side + 1) * half]

    part = jax.ShapeDtypeStruct((side_rows, PIECE + STAT), F32)
    return call(
        kernel,
        (part, part),
        (near, far, keys, values),
        [VMEM] * 4,
        limit=8,
    )


def join_blocks(kept, swapped):
    side_rows = kept.shape[0]
    slots = side_rows // HK

    def kernel(kept_ref, swapped_ref, out_ref):
        stat = [ref[:, PIECE:] for ref in (kept_ref, swapped_ref)]
        tops, sums = [s[:, :SLOT] for s in stat], [s[:, SLOT : 2 * SLOT] for s in stat]
        top = jnp.maximum(*tops)
        factors = [jnp.exp(t - top) for t in tops]
        total = factors[0] * sums[0] + factors[1] * sums[1]
        parts = []
        for g in range(GROUP):
            cols = pl.ds(g * DH, DH)
            parts.append(
                kept_ref[:, cols] * factors[0][:, g : g + 1]
                + swapped_ref[:, cols] * factors[1][:, g : g + 1]
            )
        lane = iotas((side_rows, STAT))[1]
        field, head = div(lane, SLOT), mod(lane, SLOT)
        tops = by_row(head, [top[:, g : g + 1] for g in range(GROUP)])
        sums = by_row(head, [total[:, g : g + 1] for g in range(GROUP)])
        high = tops.astype(BF16).astype(F32)
        middle = (tops - high).astype(BF16).astype(F32)
        low = tops - high - middle
        sum_high = sums.astype(BF16).astype(F32)
        parts.append(by_row(field, [high, middle, low, sum_high, sums - sum_high]))
        packed = jnp.concatenate(parts, axis=1).astype(BF16)
        row, col = iotas((side_rows, side_rows))
        chip, k, c = div(row, HK * CAPP), mod(div(row, CAPP), HK), mod(row, CAPP)
        out_ref[...] = dot(one_hot(k * slots + chip * CAPP + c == col), packed).astype(BF16)

    return call(
        kernel,
        pltpu.VMEM((side_rows, PIECE + STAT), BF16),
        (kept, swapped),
        [VMEM, VMEM],
        limit=4,
        out_specs=VMEM,
    )


def routes_out(named, pack_ref):
    rows = len(named[0])
    row, col = iotas((EXPERTS * SLOT, HK * rows))
    expert, i, k, r = div(row, SLOT), mod(row, SLOT), div(col, rows), mod(col, rows)
    has = (by_row(r, named[0]) == expert) | (by_row(r, named[1]) == expert)
    a, b = iotas((HK * rows, HK * rows))
    earlier = (div(a, rows) == div(b, rows)) & (mod(a, rows) < mod(b, rows))
    rank = dot(one_hot(has), one_hot(earlier)).astype(jnp.int32)
    for n in range(BLOCKS):
        slot = jnp.where(i < CAPE, i, (i - CAPE) * PER + n)
        piece = jnp.where(i < CAPE, n, HK - 1)
        pack_ref[n] = one_hot(has & (rank == slot) & (k == piece))


def routes_back(named, logits, half, main_ref, tail_ref, gate_ref):
    rows = len(named[0])
    per_expert = half // EXPERTS
    row, col = iotas((2 * rows, half * SLOT))
    j, r = div(row, rows), mod(row, rows)
    expert, i = div(div(col, SLOT), per_expert), mod(col, SLOT)
    mine = jnp.where(j == 0, by_row(r, named[0]), by_row(r, named[1]))
    rank = jnp.zeros(row.shape, jnp.int32)
    for q in range(rows):
        same = (mine == named[0][q]) | (mine == named[1][q])
        rank += ((r > q) & same).astype(jnp.int32)
    here = expert == mine
    main_ref[...] = one_hot(here & (i == rank))
    for n in range(BLOCKS):
        spot = jnp.full(row.shape, -1, jnp.int32)
        for m in range(SLOT - CAPE):
            spot = jnp.where(rank == m * PER + n, CAPE + m, spot)
        tail_ref[n] = one_hot(here & (i == spot))

    row, _ = iotas((rows, STAT))
    first, second = by_row(row, logits[0]), by_row(row, logits[1])
    top = jnp.maximum(first, second)
    first, second = jnp.exp(first - top), jnp.exp(second - top)
    gate_ref[0] = first / (first + second)
    gate_ref[1] = second / (first + second)


def own_experts(expert_ref, start, rows):
    return [[expert_ref[j, start + r] for r in range(rows)] for j in range(2)]


def stage(prefix_of, expert_index, lengths, arrays, after, devices, rows, span):
    half = devices // 2
    holders = half // PREFIXES
    expert_index = expert_index.T
    count = len(arrays)

    def kernel(*refs):
        _, prefix_hbm, expert_hbm, length_hbm = refs[:4]
        sources, outs = refs[4 : 4 + count], refs[4 + count : 4 + 2 * count]
        find_ref, pack_ref, live_ref, prefix_ref, expert_ref, length_ref, sems = refs[4 + 2 * count :]
        copies = fetch(
            [
                (prefix_hbm, prefix_ref), (expert_hbm, expert_ref), (length_hbm, length_ref),
                *zip(sources, outs),
            ],
            sems,
        )
        start = lax.axis_index("wide") * rows
        for copy in copies[:3]:
            copy.wait()
        row, col = iotas((rows, rows * span))
        owner = div(col, span)
        length = by_row(owner, [length_ref[r] for r in range(rows)])
        live_ref[...] = ((owner == row) & (mod(col, span) < length)).astype(F32)
        named, ranks = prefix_slots(prefix_ref, start, rows)
        firsts = [named[r] * (holders * HK * CAPP) + ranks[r] for r in range(rows)]
        row, col = iotas((HK * rows, half * HK * CAPP))
        target = by_row(mod(row, rows), firsts) + div(row, rows) * CAPP
        for h in range(holders):
            find_ref[h] = one_hot(target + h * (HK * CAPP) == col)
        routes_out(own_experts(expert_ref, start, rows), pack_ref)
        for copy in copies[3:]:
            copy.wait()

    return call(
        kernel,
        (
            *[pltpu.VMEM(x.shape, x.dtype) for x in arrays],
            pltpu.VMEM((holders, HK * rows, half * HK * CAPP), BF16),
            pltpu.VMEM((BLOCKS, EXPERTS * SLOT, HK * rows), BF16),
            pltpu.VMEM((rows, rows * span), F32),
        ),
        (after, prefix_of, expert_index, lengths, *arrays),
        [VMEM] + [HBM] * (3 + count),
        flops=1 << 30,
        scratch=[
            pltpu.SMEM(prefix_of.shape, jnp.int32),
            pltpu.SMEM(expert_index.shape, jnp.int32),
            pltpu.SMEM(lengths.shape, jnp.int32),
            pltpu.SemaphoreType.DMA((3 + count,)),
        ],
        out_specs=(VMEM,) * (3 + count),
        limit=4,
    )


def suffix_block(queries, keys, values, live, after):
    rows = queries.shape[0]

    def kernel(_, query_ref, key_ref, value_ref, live_ref, out_ref, stat_ref):
        own_suffix(
            query_ref[...].astype(F32), key_ref, value_ref, live_ref[...], out_ref, stat_ref
        )

    return call(
        kernel,
        (pltpu.VMEM((HK * rows, PIECE), F32), pltpu.VMEM((HK * rows, STAT), F32)),
        (after, queries, keys, values, live),
        [VMEM] * 5,
        flops=1 << 30,
        out_specs=(VMEM, VMEM),
        limit=4,
    )


def finish(attended, expert_index, gate_logits, after, devices):
    rows = attended.shape[0]
    half = devices // 2
    expert_index, gate_logits = expert_index.T, gate_logits.T

    def kernel(
        _, attended_ref, expert_hbm, logit_hbm,
        out_hbm, main_ref, tail_ref, gate_ref, expert_ref, logit_ref, sems,
    ):
        copies = fetch(
            [(expert_hbm, expert_ref), (logit_hbm, logit_ref), (attended_ref, out_hbm)], sems
        )
        start = lax.axis_index("wide") * rows
        for copy in copies[:2]:
            copy.wait()
        named = own_experts(expert_ref, start, rows)
        logits = own_experts(logit_ref, start, rows)
        routes_back(named, logits, half, main_ref, tail_ref, gate_ref)
        copies[2].wait()

    return call(
        kernel,
        (
            pltpu.HBM(attended.shape, attended.dtype),
            pltpu.VMEM((2 * rows, half * SLOT), BF16),
            pltpu.VMEM((BLOCKS, 2 * rows, half * SLOT), BF16),
            pltpu.VMEM((2, rows, STAT), F32),
        ),
        (after, attended, expert_index, gate_logits),
        [VMEM, VMEM, HBM, HBM],
        flops=1 << 30,
        scratch=[
            pltpu.SMEM(expert_index.shape, jnp.int32),
            pltpu.SMEM(gate_logits.shape, F32),
            pltpu.SemaphoreType.DMA((3,)),
        ],
        out_specs=(HBM, VMEM, VMEM, VMEM),
        limit=4,
    )


def merge(back, suffix_out, suffix_stat, hidden_in, gain, find, pack, devices):
    rows, width = hidden_in.shape
    half = devices // 2
    per_expert = half // EXPERTS

    def kernel(
        back_ref, suffix_ref, stat_ref, hidden_ref, gain_ref, find_ref, pack_ref, out_ref, sent_ref
    ):
        stat = stat_ref[...]
        outs, tops, sums = [suffix_ref[...]], [stat[:, :SLOT]], [stat[:, SLOT : 2 * SLOT]]
        for h in range(find_ref.shape[0]):
            found = dot(find_ref[h], back_ref[...])
            stat = found[:, PIECE:]
            field = [stat[:, n * SLOT : (n + 1) * SLOT] for n in range(5)]
            outs.append(found[:, :PIECE])
            tops.append(field[0] + field[1] + field[2])
            sums.append(field[3] + field[4])
        overall = tops[0]
        for top in tops[1:]:
            overall = jnp.maximum(overall, top)
        factors = [jnp.exp(top - overall) for top in tops]
        scale = 1.0 / sum(f * s for f, s in zip(factors, sums))
        factors = [f * scale for f in factors]
        merged = []
        for g in range(GROUP):
            cols = slice(g * DH, (g + 1) * DH)
            merged.append(sum(o[:, cols] * f[:, g : g + 1] for o, f in zip(outs, factors)))
        attended = jnp.concatenate(merged, axis=1).astype(BF16).astype(F32)
        for k in range(HK):
            out_ref[:, pl.ds(k * PIECE, PIECE)] = attended[k * rows : (k + 1) * rows].astype(BF16)
        stream = stack_pieces(hidden_ref[...].astype(F32)) + attended
        squares = jnp.sum(stream * stream, axis=-1, keepdims=True)
        mean = sum(squares[k * rows : (k + 1) * rows] for k in range(HK)) * (1.0 / width)
        scale = jnp.concatenate([lax.rsqrt(mean + 1e-05)] * HK, axis=0)
        gain = jnp.concatenate(
            [
                jnp.broadcast_to(gain_ref[:, k * PIECE : (k + 1) * PIECE], (rows, PIECE))
                for k in range(HK)
            ],
            axis=0,
        )
        normed = (stream * scale * gain).astype(BF16)
        for n in range(BLOCKS):
            taken = dot(pack_ref[n], normed)
            for i in range(half):
                e = i // per_expert
                sent_ref[pl.ds(i * SLOT, SLOT), pl.ds(n * PIECE, PIECE)] = taken[
                    e * SLOT : (e + 1) * SLOT
                ].astype(BF16)

    return call(
        kernel,
        (
            pltpu.VMEM((rows, width), BF16),
            pltpu.VMEM((half * SLOT, BLOCKS * PIECE), BF16),
        ),
        (back, suffix_out, suffix_stat, hidden_in, gain, find, pack),
        [VMEM] * 7,
        limit=8,
        out_specs=(VMEM, VMEM),
    )


def cuts(total, step):
    return [(p, min(step, total - p)) for p in range(0, total, step)]


def experts(near, far, gate_weight, up_weight, down_weight):
    half = near.shape[0]
    units, width = down_weight.shape
    depth = 4
    unit_cuts = cuts(units, 512)
    out_cuts = cuts(width, 512)

    def kernel(
        near_ref, far_ref, gate_hbm, up_hbm, down_hbm, mine_ref, theirs_ref,
        gate_ref, up_ref, down_ref, rows_ref, hidden_ref, sems,
    ):
        copies = []
        for p, step in unit_cuts:
            copies.append((gate_hbm, gate_ref, pl.ds(p, step)))
            copies.append((up_hbm, up_ref, pl.ds(p, step)))
        for p, step in out_cuts:
            copies.append((down_hbm, down_ref, pl.ds(p, step)))

        def copy(n):
            source, target, cols = copies[n]
            return pltpu.make_async_copy(source.at[:, cols], target.at[:, cols], sems.at[n])

        for n in range(min(depth, len(copies))):
            copy(n).start()

        def arrive(n):
            copy(n).wait()
            if n + depth < len(copies):
                copy(n + depth).start()

        row, col = iotas((half, half))
        i, i_from = mod(row, SLOT), mod(col, SLOT)
        same = div(row, SLOT) == div(col, SLOT)
        for side, ref in enumerate((near_ref, far_ref)):
            own = pl.ds(side * half, half)
            tail = jnp.zeros((half, PIECE), F32)
            for n in range(BLOCKS):
                spot = jnp.full(row.shape, -1, jnp.int32)
                for m in range(SLOT - CAPE):
                    spot = jnp.where(i == m * PER + n, CAPE + m, spot)
                tail += dot(one_hot(same & (i_from == spot)), ref[:, n * PIECE : (n + 1) * PIECE])
            rows_ref[own, : BLOCKS * PIECE] = ref[...]
            rows_ref[own, BLOCKS * PIECE :] = tail.astype(BF16)
        for n, (p, step) in enumerate(unit_cuts):
            cols = pl.ds(p, step)
            arrive(2 * n)
            gate = dot(rows_ref[...], gate_ref[:, cols])
            arrive(2 * n + 1)
            up = dot(rows_ref[...], up_ref[:, cols])
            hidden_ref[:, cols] = (gate / (1.0 + jnp.exp(-gate)) * up).astype(BF16)
        for n, (p, step) in enumerate(out_cuts):
            cols = pl.ds(p, step)
            arrive(2 * len(unit_cuts) + n)
            part = dot(hidden_ref[...], down_ref[:, cols])
            mine_ref[:, cols] = part[:half]
            theirs_ref[:, cols] = part[half:].astype(BF16)

    part = functools.partial(jax.ShapeDtypeStruct, (half, width))
    return call(
        kernel,
        (part(F32), part(BF16)),
        (near, far, gate_weight, up_weight, down_weight),
        [VMEM, VMEM, HBM, HBM, HBM],
        flops=12 * half * units * width,
        moved=6 * units * width,
        limit=42,
        scratch=[
            pltpu.VMEM(gate_weight.shape, BF16),
            pltpu.VMEM(up_weight.shape, BF16),
            pltpu.VMEM(down_weight.shape, BF16),
            pltpu.VMEM((2 * half, width), BF16),
            pltpu.VMEM((2 * half, units), BF16),
            pltpu.SemaphoreType.DMA((2 * len(unit_cuts) + len(out_cuts),)),
        ],
    )


def add_and_pack(mine, swapped):
    half, width = mine.shape

    def kernel(mine_ref, swapped_ref, out_ref):
        row, col = iotas((half, half))
        same = div(row, SLOT) == div(col, SLOT)
        i, i_from = mod(row, SLOT), mod(col, SLOT)
        keep = mod(iotas((half, PIECE))[0], SLOT) < CAPE
        last = pl.ds(BLOCKS * PIECE, PIECE)
        tail = (mine_ref[:, last] + swapped_ref[:, last].astype(F32)).astype(BF16)
        for n in range(BLOCKS):
            cols = pl.ds(n * PIECE, PIECE)
            moved = dot(one_hot(same & (i >= CAPE) & (i_from == (i - CAPE) * PER + n)), tail)
            out_ref[:, cols] = jnp.where(keep, mine_ref[:, cols] + swapped_ref[:, cols].astype(F32), moved).astype(BF16)

    return call(
        kernel,
        jax.ShapeDtypeStruct((half, BLOCKS * PIECE), BF16),
        (mine, swapped),
        [VMEM, VMEM],
    )


def mix(parts, main, tail, gates):
    rows = main.shape[0] // 2

    def kernel(part_ref, main_ref, tail_ref, gate_ref, out_ref):
        first, second = gate_ref[0][:, :1], gate_ref[1][:, :1]
        last = jnp.zeros((2 * rows, PIECE), F32)
        for n in range(BLOCKS):
            cols = pl.ds(n * PIECE, PIECE)
            both = jnp.concatenate([main_ref[...], tail_ref[n]], axis=0)
            found = dot(both, part_ref[:, cols])
            out_ref[:, cols] = (found[:rows] * first + found[rows : 2 * rows] * second).astype(BF16)
            last += found[2 * rows :]
        cols = pl.ds(BLOCKS * PIECE, PIECE)
        out_ref[:, cols] = (last[:rows] * first + last[rows:] * second).astype(BF16)

    return call(
        kernel,
        jax.ShapeDtypeStruct((rows, HK * PIECE), BF16),
        (parts, main, tail, gates),
        [VMEM, VMEM, VMEM, VMEM],
    )


def exchange(x, groups):
    return lax.all_to_all(x, "wide", 0, 0, tiled=True, axis_index_groups=groups)


def local(
    queries,
    hidden_in,
    prefix_keys,
    prefix_values,
    suffix_keys,
    suffix_values,
    suffix_length,
    prefix_of,
    expert_index,
    gate_logits,
    norm_gain,
    gate_weight,
    up_weight,
    down_weight,
):
    devices = lax.axis_size("wide")
    rows = queries.shape[0]
    half = devices // 2
    siblings = [(i, i ^ 1) for i in range(devices)]
    alike = [[2 * i + c for i in range(half)] for c in range(2)]
    prefix_of = prefix_of[:, 0]

    outgoing = send_queries(queries, prefix_of, devices)
    near = exchange(outgoing, alike)
    far = lax.ppermute(near, "wide", siblings)
    flat = (-1, suffix_keys.shape[2])
    keys, values, suffix_keys, suffix_values, own, hidden, gain, find, pack, live = stage(
        prefix_of,
        expert_index,
        suffix_length,
        (
            prefix_keys, prefix_values, suffix_keys.reshape(flat), suffix_values.reshape(flat),
            queries, hidden_in, norm_gain.reshape(1, -1),
        ),
        near,
        devices,
        rows,
        suffix_keys.shape[1],
    )
    kept, given = prefix_block(near, far, keys, values)
    swapped = lax.ppermute(given, "wide", siblings)
    suffix_out, suffix_stat = suffix_block(own, suffix_keys, suffix_values, live, kept)
    swapped, suffix_stat = lax.optimization_barrier((swapped, suffix_stat))
    back = exchange(join_blocks(kept, swapped), alike)
    attended, sent = merge(back, suffix_out, suffix_stat, hidden, gain, find, pack, devices)
    near = exchange(sent, alike)
    far = lax.ppermute(near, "wide", siblings)
    attended, main, tail, gates = finish(attended, expert_index, gate_logits, near, devices)
    far, gates = lax.optimization_barrier((far, gates))
    mine, theirs = experts(near, far, gate_weight, up_weight, down_weight)
    swapped = lax.ppermute(theirs, "wide", siblings)
    parts = exchange(add_and_pack(mine, swapped), alike)
    return attended, mix(parts, main, tail, gates)


def solution(mesh):
    placed = (
        P(("groups", "wide"), None),
        P(("groups", "wide"), None),
        P(("groups", "wide"), None),
        P(("groups", "wide"), None),
        P(("groups", "wide"), None, None),
        P(("groups", "wide"), None, None),
        P(("groups", "wide")),
        P("groups", None),
        P("groups", None),
        P("groups", None),
        P(),
        P(None, "wide"),
        P(None, "wide"),
        P("wide", None),
    )
    return jax.shard_map(
        local,
        mesh=mesh,
        in_specs=placed,
        out_specs=(P(("groups", "wide"), None), P(("groups", "wide"), None)),
        check_vma=False,
    )
```
